512 devices in a mesh: group: 16 (over y, x), member: 32 (over z, core).
Axes of the slice: x: 4, y: 4, z: 16, core: 2. Of those that a mesh axis runs over, the one named last changes fastest.
Arguments:
- tokens: bfloat16 [65536, 2048], P(('group', 'member')), may hold values from -6 to 6
- cotangent: bfloat16 [65536, 2048], P(('group', 'member')), may hold values from -6 to 6
- w_gate: bfloat16 [2048, 512], P('member'), may hold values from -0.125 to 0.125
- w_up: bfloat16 [2048, 512], P('member'), may hold values from -0.125 to 0.125
- w_down: bfloat16 [2048, 512], P('member'), may hold values from -0.125 to 0.125
- basis: float32 [2048, 256], P('member'), may hold values from -0.088388348 to 0.088388348
- first_moment: float32 [3, 256, 512], P(None, 'member'), may hold values from -3 to 3
- second_moment: float32 [3, 256, 512], P(None, 'member'), may hold values from 0.1 to 2
Outputs:
- input_grad: bfloat16 [65536, 2048], P(('group', 'member'))
- new_first: float32 [3, 256, 512], P(None, 'member')
- new_second: float32 [3, 256, 512], P(None, 'member')
- updates: float32 [3, 2048, 512], P(None, 'member')
The draws below stay inside these ranges and needn't reach their ends.
All inputs are finite; a program needn't handle non-finite values.
Results may differ from the reference program's by a relative error of at most 0.008.
Values may be sent and summed in bfloat16 or wider, within the bound.
A program may use at most 64 MiB of HBM per device.

```python
import math
import jax
import jax.numpy as jnp
from jax import lax

D = 2048
FF = 512
RANK = 256
TOK_DEV = 128
TOKENS = 65536
N_GROUP = 16
N_MEMBER = 32


def draw_basis(key, part):
    noise_key = jax.random.fold_in(key, 11)
    position = jnp.arange(RANK, dtype=jnp.float32) / max(RANK - 1, 1)
    values = jax.random.normal(noise_key, (D, RANK), jnp.float32)
    values = jnp.clip(values, -6.0, 6.0)
    column = 1.0 + 2.0 * position
    edge = 4.0 / jnp.sqrt(jnp.float32(D))
    scaled = values * column[None, :] / jnp.sqrt(jnp.float32(D))
    return jnp.clip(scaled, -edge, edge)


def block_scale(rng, extent, shards, smallest, high):
    def one(dim, parts):
        heights = jax.random.uniform(jax.random.fold_in(jax.random.fold_in(rng, 6), dim), (parts,), jnp.float32, smallest / len(shards), high / len(shards))
        return jnp.repeat(jnp.exp(heights), extent[dim] // parts).reshape((-1,) + (1,) * (len(extent) - dim - 1))

    gain = one(*shards[0])
    for cut in shards[1:]:
        gain = gain * one(*cut)
    return gain


def gaussian(rng, extent, spread, most, split=(), kind=jnp.bfloat16):
    array = jax.random.normal(rng, extent, jnp.float32) * spread
    if len(split) > 0:
        array = block_scale(rng, extent, split, -0.22, 0.18) * array
    return jnp.clip(array, min=-most, max=most).astype(kind)


def setup_inputs(seed: int = 0) -> dict:
    seeds = jax.random.split(jax.random.key(seed), 9)
    tokens = gaussian(seeds[0], (TOKENS, D), 1.0, 6.0, ((0, 512),))
    cotangent = gaussian(seeds[1], (TOKENS, D), 1.0, 6.0, ((0, 512),))
    w_gate = gaussian(seeds[2], (D, FF), D ** -0.5, 0.125, ((0, 32),))
    w_up = gaussian(seeds[3], (D, FF), D ** -0.5, 0.125, ((0, 32),))
    w_down = gaussian(seeds[4], (D, FF), D ** -0.5, 0.125, ((0, 32),))
    basis = draw_basis(jax.random.fold_in(seeds[8], 71), 0)
    first_moment = gaussian(seeds[6], (3, RANK, FF), 0.5, 3.0, ((1, 32),), jnp.float32)
    second_moment = jnp.clip(jnp.exp(math.log(2.0) - 2.9957323 * jax.random.uniform(seeds[7], (3, RANK, FF), jnp.float32) ** block_scale(seeds[7], (3, RANK, FF), ((1, 32),), -0.2, 0.2)), 0.1, 2.0)
    return {"tokens": tokens, "cotangent": cotangent, "w_gate": w_gate, "w_up": w_up, "w_down": w_down, "basis": basis, "first_moment": first_moment, "second_moment": second_moment}


def reference(tokens, cotangent, w_gate, w_up, w_down, basis, first_moment, second_moment):
    count = N_GROUP * N_MEMBER
    x_blocks = tokens.reshape(count, TOK_DEV, D)
    y_blocks = cotangent.reshape(count, TOK_DEV, D)

    def one_block(carry, pair):
        x_rows, y_rows = pair
        gate = jnp.dot(x_rows, w_gate, preferred_element_type=jnp.float32)
        up = jnp.dot(x_rows, w_up, preferred_element_type=jnp.float32)
        sig = jax.nn.sigmoid(gate)
        silu = gate * sig
        hidden = (silu * up).astype(jnp.bfloat16)
        dhid = jnp.dot(y_rows, w_down, preferred_element_type=jnp.float32)
        dgate = (dhid * up * sig * (1.0 + gate * (1.0 - sig))).astype(jnp.bfloat16)
        dup = (dhid * silu).astype(jnp.bfloat16)
        dx = lax.dot_general(dgate, w_gate, (((1,), (1,)), ((), ())), preferred_element_type=jnp.float32)
        dx = dx + lax.dot_general(dup, w_up, (((1,), (1,)), ((), ())), preferred_element_type=jnp.float32)
        grad_gate = lax.dot_general(x_rows, dgate, (((0,), (0,)), ((), ())), preferred_element_type=jnp.float32)
        grad_up = lax.dot_general(x_rows, dup, (((0,), (0,)), ((), ())), preferred_element_type=jnp.float32)
        grad_down = lax.dot_general(y_rows, hidden, (((0,), (0,)), ((), ())), preferred_element_type=jnp.float32)
        carry = carry + jnp.stack([grad_gate, grad_up, grad_down])
        return (carry, dx.astype(jnp.bfloat16))
    start = jnp.zeros((3, D, FF), jnp.float32)
    grads, dx_blocks = lax.scan(one_block, start, (x_blocks, y_blocks))
    input_grad = dx_blocks.reshape(TOKENS, D)
    lowrank = jnp.einsum('dr,kdf->krf', basis, grads, precision=lax.Precision.HIGHEST)
    limit = math.sqrt(3.0 * RANK * FF)
    factor = jnp.minimum(1.0, limit / jnp.sqrt(jnp.sum(lowrank * lowrank) + 1e-06))
    grad_low = factor * lowrank
    new_first = 0.5 * first_moment + 0.5 * grad_low
    new_second = 0.9 * second_moment + 0.1 * grad_low * grad_low
    step = (new_first / (jnp.sqrt(new_second) + 1e-08)).astype(jnp.bfloat16)
    updates = jnp.einsum('dr,krf->kdf', basis, step.astype(jnp.float32), precision=lax.Precision.HIGHEST)
    return (input_grad, new_first, new_second, updates)
```

```python
import functools
import math

import jax
import jax.numpy as jnp
from jax import lax
from jax.experimental import pallas as pl
from jax.experimental.pallas import tpu as pltpu
from jax.sharding import PartitionSpec as P

BF = jnp.bfloat16
F32 = jnp.float32
MESH = pl.DeviceIdType.MESH

D = 2048
FF = 512
RANK = 256
TOK = 128
NX, NY, NZ = 4, 4, 16
NP = NX * NY
HF = FF // 2
HR = RANK // 2
ROWS = 64
PW = 3 * HF + HR
EPS_LIMIT = math.sqrt(3.0 * RANK * FF)

G0, U0, B0, D0 = 0, HF, 2 * HF, 2 * HF + HR


class Sems:
    def __init__(self, ref, count):
        self.ref, self.count, self.used = ref, count, 0

    def take(self):
        self.used += 1
        assert self.used <= self.count
        return self.ref.at[self.used - 1]


NSEND = 240


def kernel(
    tok_hbm, cot_hbm, wg_hbm, wu_hbm, wd_hbm, bas_hbm, fm_hbm, sm_hbm,
    dx_hbm, nf_hbm, ns_hbm, up_hbm,
    toks, cots, wbuf, wgv, wuv, wdv, basv, fmv, smv,
    pk, bp, msend, mrecv, mbuf,
    accx, accy, xpb, dgu, hid, lsend, lrecv,
    dxp, dxr, dxo, t0b, nearb, t1b, farb,
    sqo, sqp, sqb, lrow, lall, loth, sbuf, uov, ucv, nfv, nsv,
    lsem, ssem, zsem, xysem, psem, msem, rsem, nsem, fsem, qsem, rowsem, stsem,
):
    g = lax.axis_index("group")
    m = lax.axis_index("member")
    y, x = lax.div(g, NX), lax.rem(g, NX)
    z, c = lax.div(m, 2), lax.rem(m, 2)
    o = 1 - c
    p = g

    def dev(dx=0, dy=0, dz=0):
        yy = lax.rem(y + dy + NY, NY)
        xx = lax.rem(x + dx + NX, NX)
        zz = lax.rem(z + dz + NZ, NZ)
        return (yy * NX + xx, zz * 2 + c)

    partner = (g, z * 2 + o)

    local = []

    def load(src, dst):
        cp = pltpu.make_async_copy(src, dst, lsem.at[len(local)])
        cp.start()
        local.append(cp)
        return cp

    ld_w = [load(wg_hbm, wgv), load(wu_hbm, wuv), load(wd_hbm, wdv), load(bas_hbm, basv)]
    ld_t = [load(tok_hbm, toks.at[c]), load(cot_hbm, cots.at[c])]
    ld_m = [load(fm_hbm, fmv), load(sm_hbm, smv)]

    barrier = pltpu.get_barrier_semaphore()
    near = [partner]
    near += [dev(dz=1), dev(dz=-1), dev(dz=2), dev(dz=-2)]
    near += [dev(dx=1), dev(dx=-1), dev(dx=2)]
    near += [dev(dy=1), dev(dy=-1), dev(dy=2)]
    for d in near:
        pl.semaphore_signal(barrier, inc=1, device_id=d, device_id_type=MESH)

    sends = []
    takes = Sems(ssem, NSEND)

    def remote(src, dst, rsem_, d):
        cp = pltpu.make_async_remote_copy(
            src_ref=src, dst_ref=dst, send_sem=takes.take(), recv_sem=rsem_,
            device_id=d, device_id_type=MESH,
        )
        cp.start()
        sends.append(cp)
        return cp

    def arrived(dst, rsem_):
        pltpu.make_async_remote_copy(
            src_ref=dst, dst_ref=dst, send_sem=ssem.at[0], recv_sem=rsem_,
            device_id=partner, device_id_type=MESH,
        ).wait_recv()

    for cp in ld_w:
        cp.wait()
    pr = lax.broadcasted_iota(jnp.int32, (RANK, RANK), 0)
    pc = lax.broadcasted_iota(jnp.int32, (RANK, RANK), 1)
    perm = (pr == (pc & (NZ - 1)) * NP + (pc >> 4)).astype(F32).astype(BF)
    bas = basv[...]
    bh = bas.astype(BF)
    bl = (bas - bh.astype(F32)).astype(BF)
    bp[c, 0] = jnp.dot(bh, perm, preferred_element_type=F32).astype(BF)
    bp[c, 1] = jnp.dot(bl, perm, preferred_element_type=F32).astype(BF)

    def al(v, n):
        return pl.multiple_of(v, n)

    own_rows = pl.ds(al(c * ROWS, ROWS), ROWS)
    for half, put in ((o, "partner"), (c, "own")):
        fs = pl.ds(al(half * HF, HF), HF)
        rs = pl.ds(al(half * HR, HR), HR)
        for col, width, val in (
            (G0, HF, wgv[:, fs]), (U0, HF, wuv[:, fs]), (B0, HR, bp[c, 0, :, rs]), (D0, HF, wdv[:, fs]),
        ):
            if put == "partner":
                pk[:, col : col + width] = val
            else:
                wbuf[z, own_rows, col : col + width] = val

    pl.semaphore_wait(barrier, len(near))

    remote(pk, wbuf.at[z, own_rows], psem.at[0], partner)

    def roff(h, dx=0, dy=0):
        if h == 0:
            return al(16 * lax.rem(x + dx + NX, NX), 16)
        return al(64 + 16 * lax.rem(y + dy + NY, NY), 16)

    def zchunk(zo, row):
        return wbuf.at[zo, pl.ds(row, 16)]

    def zsend(zo, h, row, dz, rel):
        remote(zchunk(zo, row), zchunk(zo, row), zsem.at[h, rel], dev(dz=dz))

    own_off = al((1 - c) * (16 * x) + c * (64 + 16 * y), 16)
    oth_off = al(c * (16 * x) + (1 - c) * (64 + 16 * y), 16)
    for h, off in ((c, own_off), (o, oth_off)):
        if h is o:
            arrived(wbuf.at[z, pl.ds(al(o * ROWS, ROWS), ROWS)], psem.at[0])
        for dz in (1, -1, 2, -2):
            zsend(z, h, off, dz, dz % NZ)

    for cp in ld_t:
        cp.wait()
    remote(toks.at[c], toks.at[c], psem.at[1], partner)
    remote(cots.at[c], cots.at[c], psem.at[2], partner)
    remote(bp.at[c], bp.at[c], psem.at[3], partner)

    for cp in ld_m:
        cp.wait()
    prow = lax.rem(p, 8)
    pcore = lax.div(p, 8)
    zero = jnp.zeros((2, HF), F32)
    msend[6:8, :] = zero
    mbuf[z, 6:8, :] = zero
    for i, mv in enumerate((fmv, smv)):
        for k in range(3):
            msend[3 * i + k : 3 * i + k + 1, :] = mv[k, pl.ds(prow, 1), pl.ds(al(o * HF, HF), HF)]
            mbuf[z, 3 * i + k : 3 * i + k + 1, :] = mv[k, pl.ds(prow, 1), pl.ds(al(c * HF, HF), HF)]
    remote(msend, mrecv, psem.at[4], partner)

    def origin(rel):
        return lax.rem(z - rel + NZ, NZ)

    def z_arrive(s):
        for d in (0, 1):
            rel = s if d == 0 else NZ - s
            zo = origin(rel)
            sgn = 1 if d == 0 else -1
            hs = (0, 1) if s < 8 else ((0,) if d == 0 else (1,))
            for h in hs:
                arrived(zchunk(zo, roff(h)), zsem.at[h, rel])
                if s % 2 == 0 and s < 8:
                    zsend(zo, h, roff(h), sgn, (rel + sgn) % NZ)
                    if s + 2 < 8 or (d == 0) == (h == 0):
                        zsend(zo, h, roff(h), 2 * sgn, (rel + 2 * sgn) % NZ)
            for h in hs:
                for e in (1, -1):
                    t = dev(dx=e) if h == 0 else dev(dy=e)
                    remote(zchunk(zo, roff(h)), zchunk(zo, roff(h)), xysem.at[h, 0 if e == 1 else 1, rel], t)

    def pieces(s):
        if s == 8:
            return [(8, (0, 1))]
        return [(s, (0, 0)), (NZ - s, (1, 1))]

    def step_of(h, e):
        return roff(h, dx=e) if h == 0 else roff(h, dy=e)

    def xy_direct(s):
        for rel, ways in pieces(s):
            zo = origin(rel)
            for h in (0, 1):
                way = ways[h]
                e = -1 if way == 0 else 1
                ch = zchunk(zo, step_of(h, e))
                arrived(ch, xysem.at[h, way, rel])
                t = dev(dx=-e) if h == 0 else dev(dy=-e)
                remote(ch, ch, xysem.at[h, 2, rel], t)

    def xy_rest(s):
        for rel, ways in pieces(s):
            zo = origin(rel)
            for h in (0, 1):
                way = 1 - ways[h]
                e = -1 if way == 0 else 1
                arrived(zchunk(zo, step_of(h, e)), xysem.at[h, way, rel])
                arrived(zchunk(zo, step_of(h, 2)), xysem.at[h, 2, rel])

    def multiply(rel, first=False):
        zo = origin(rel)
        cols = pl.ds(al(zo * 128, 128), 128)
        tk = toks[:, :, cols].reshape(2 * TOK, 128)
        ck = cots[:, :, cols].reshape(2 * TOK, 128)
        ax = jnp.dot(tk, wbuf[zo, :, 0:D0], preferred_element_type=F32)
        ay = jnp.dot(ck, wbuf[zo, :, B0:PW], preferred_element_type=F32)
        if first:
            accx[...] = ax
            accy[...] = ay
        else:
            accx[...] += ax
            accy[...] += ay

    def finish(s):
        xy_rest(s)
        for rel, _ in pieces(s):
            multiply(rel)

    for s in range(1, 9):
        z_arrive(s)
        if s == 6:
            arrived(mrecv, psem.at[4])
            mine = pcore == c
            mbuf[z] = jnp.where(mine, mbuf[z], mrecv[...])
            for dz in range(1, NZ):
                remote(mbuf.at[z], mbuf.at[z], msem.at[dz], dev(dz=dz))
        if s > 1:
            xy_direct(s - 1)
        if s == 2:
            other = 1 - c
            arrived(toks.at[other], psem.at[1])
            arrived(cots.at[other], psem.at[2])
            multiply(0, first=True)
        if s > 3:
            finish(s - 3)
    xy_direct(8)
    for s in (6, 7, 8):
        finish(s)

    hc = pl.ds(al(c * HR, HR), HR)
    ho = pl.ds(al(o * HR, HR), HR)
    xpb[0, :, hc] = accx[:, B0 : B0 + HR].astype(BF)
    xpb[1, :, hc] = accy[:, 0:HR].astype(BF)
    remote(xpb.at[:, :, hc], xpb.at[:, :, hc], psem.at[5], partner)
    gate = accx[:, G0 : G0 + HF]
    up = accx[:, U0 : U0 + HF]
    dhid = accy[:, HR : HR + HF]
    sig = jax.nn.sigmoid(gate)
    silu = gate * sig
    hid[...] = (silu * up).astype(BF)
    dgu[:, 0:HF] = (dhid * up * sig * (1.0 + gate * (1.0 - sig))).astype(BF)
    dgu[:, HF : 2 * HF] = (dhid * silu).astype(BF)
    arrived(xpb.at[:, :, ho], psem.at[5])

    over_rows = (((0,), (0,)), ((), ()))
    l01 = lax.dot_general(xpb[0], dgu[...], over_rows, preferred_element_type=F32)
    lsend[0] = l01[:, 0:HF].astype(BF)
    lsend[1] = l01[:, HF : 2 * HF].astype(BF)
    lsend[2] = lax.dot_general(xpb[1], hid[...], over_rows, preferred_element_type=F32).astype(BF)

    plane = [(dx, dy) for dy in range(NY) for dx in range(NX) if (dx, dy) != (0, 0)]
    far_first = sorted(plane, key=lambda t: -(min(t[0], NX - t[0]) + min(t[1], NY - t[1])))

    def back(dx, dy):
        return ((-dy) % NY) * NX + (-dx) % NX

    def part_of(dx, dy):
        return lax.rem(y + dy, NY) * NX + lax.rem(x + dx, NX)

    def rows_of(q):
        return pl.ds(al(q * NZ, NZ), NZ)

    for dx, dy in far_first:
        q = part_of(dx, dy)
        remote(lsend.at[:, rows_of(q)], lrecv.at[p], rsem.at[back(dx, dy)], dev(dx=dx, dy=dy))
    lrecv[p] = lsend[:, rows_of(p)]

    def dx_of(core, out):
        rows = pl.ds(al(core * TOK, TOK), TOK)
        lhs = dgu[rows, :]

        @pl.loop(0, NZ)
        def _(i):
            out[:, pl.ds(al(i * 128, 128), 128)] = lax.dot_general(
                lhs, wbuf[i, :, 0 : 2 * HF], (((1,), (1,)), ((), ())), preferred_element_type=F32
            )

    dx_of(o, dxp)
    remote(dxp, dxr, psem.at[6], partner)

    def sum_parts(own, bufs):
        total = own
        for b in bufs:
            total = total + b.astype(F32)
        return total

    for dx, dy in plane:
        arrived(lrecv.at[part_of(dx, dy)], rsem.at[dy * NX + dx])
    total = lrecv[0].astype(F32)
    for q in range(1, NP):
        total = total + lrecv[q].astype(F32)
    t0b[...] = total.astype(BF)
    for i, dz in enumerate((1, -1, -2)):
        remote(t0b, nearb.at[i], nsem.at[i], dev(dz=dz))
    for i in range(3):
        arrived(nearb.at[i], nsem.at[i])
    total = sum_parts(total, [nearb[i] for i in range(3)])
    t1b[...] = total.astype(BF)
    for i, dz in ((2, 8), (0, 4), (1, -4)):
        remote(t1b, farb.at[i], fsem.at[i], dev(dz=dz))

    rows = pl.ds(al(c * TOK, TOK), TOK)
    arrived(dxr, psem.at[6])
    lhs_own = dgu[rows, :]

    @pl.loop(0, NZ)
    def _(i):
        cols = pl.ds(al(i * 128, 128), 128)
        part = lax.dot_general(
            lhs_own, wbuf[i, :, 0 : 2 * HF], (((1,), (1,)), ((), ())), preferred_element_type=F32
        )
        dxo[:, cols] = (part + dxr[:, cols]).astype(BF)

    outs = []

    def store(src, dst):
        cp = pltpu.make_async_copy(src, dst, lsem.at[8 + len(outs)])
        cp.start()
        outs.append(cp)

    store(dxo, dx_hbm)

    for i in range(3):
        arrived(farb.at[i], fsem.at[i])
    total = sum_parts(total, [farb[i] for i in range(3)])

    sq = jnp.sum(jnp.sum(total * total, axis=0), axis=0, keepdims=True)
    sq = jnp.sum(sq, axis=1, keepdims=True)
    sqo[...] = jnp.broadcast_to(sq, (1, HF))
    remote(sqo, sqp, psem.at[7], partner)
    zrow = lax.broadcasted_iota(jnp.int32, (3, NZ, HF), 1) == z
    mine3 = jnp.sum(jnp.where(zrow, total, 0.0), axis=1)
    lrow[0:3, :] = mine3
    lrow[3:8, :] = jnp.zeros((5, HF), F32)
    arrived(sqp, psem.at[7])
    sqb[p] = sqo[...] + sqp[...]
    for dx, dy in far_first:
        remote(sqb.at[p], sqb.at[p], qsem.at[back(dx, dy)], dev(dx=dx, dy=dy))
    lall[p] = lrow[...]
    for dx, dy in far_first:
        remote(lrow, lall.at[p], rowsem.at[back(dx, dy)], dev(dx=dx, dy=dy))
    for dz in range(1, NZ):
        arrived(mbuf.at[origin(dz)], msem.at[dz])
    for dx, dy in plane:
        arrived(sqb.at[part_of(dx, dy)], qsem.at[dy * NX + dx])
    ssum = sqb[0]
    for q in range(1, NP):
        ssum = ssum + sqb[q]
    factor = jnp.minimum(1.0, EPS_LIMIT / jnp.sqrt(ssum + 1e-06))

    def adam(low, first, second):
        grad = factor * low
        nf = 0.5 * first + 0.5 * grad
        ns = 0.9 * second + 0.1 * grad * grad
        return nf, ns

    for k in range(3):
        nf, ns = adam(total[k], mbuf[:, k, :], mbuf[:, 3 + k, :])
        sbuf[k, rows_of(p), :] = (nf / (jnp.sqrt(ns) + 1e-08)).astype(BF)
    for dx, dy in far_first:
        mine = sbuf.at[:, rows_of(p)]
        remote(mine, mine, stsem.at[back(dx, dy)], dev(dx=dx, dy=dy))

    for dx, dy in plane:
        arrived(lall.at[part_of(dx, dy)], rowsem.at[dy * NX + dx])
    remote(lall.at[pl.ds(al(o * 8, 8), 8)], loth, psem.at[8], partner)
    fc = pl.ds(al(c * HF, HF), HF)
    fo = pl.ds(al(o * HF, HF), HF)
    for k in range(3):
        nf, ns = adam(lall[pl.ds(al(c * 8, 8), 8), k, :], fmv[k, :, fc], smv[k, :, fc])
        nfv[k, :, fc] = nf
        nsv[k, :, fc] = ns
    arrived(loth, psem.at[8])
    for k in range(3):
        nf, ns = adam(loth[:, k, :], fmv[k, :, fo], smv[k, :, fo])
        nfv[k, :, fo] = nf
        nsv[k, :, fo] = ns
    store(nfv, nf_hbm)
    store(nsv, ns_hbm)

    arrived(bp.at[o], psem.at[3])
    for dx, dy in plane:
        arrived(sbuf.at[:, rows_of(part_of(dx, dy))], stsem.at[dy * NX + dx])

    def update(core, k):
        st = sbuf[k]
        return jnp.dot(bp[core, 0], st, preferred_element_type=F32) + jnp.dot(
            bp[core, 1], st, preferred_element_type=F32
        )

    for k in range(3):
        uov[k] = update(o, k)
    remote(uov, up_hbm.at[:, :, fc], psem.at[9], partner)
    for k in range(3):
        ucv[k] = update(c, k)
    store(ucv, up_hbm.at[:, :, fc])
    arrived(up_hbm.at[:, :, fo], psem.at[9])
    for cp in outs:
        cp.wait()
    for cp in sends:
        cp.wait_send()


def local(tokens, cotangent, w_gate, w_up, w_down, basis, first_moment, second_moment):
    anywhere = pl.BlockSpec(memory_space=pl.ANY)
    dma = pltpu.SemaphoreType.DMA
    v = pltpu.VMEM
    part = (3, NZ, HF)
    scratch = [
        v((2, TOK, D), BF), v((2, TOK, D), BF), v((NZ, 128, PW), BF),
        v((ROWS, FF), BF), v((ROWS, FF), BF), v((ROWS, FF), BF), v((ROWS, RANK), F32),
        v((3, 8, FF), F32), v((3, 8, FF), F32),
        v((ROWS, PW), BF), v((2, 2, ROWS, RANK), BF),
        v((8, HF), F32), v((8, HF), F32), v((NZ, 8, HF), F32),
        v((2 * TOK, D0), F32), v((2 * TOK, HR + HF), F32),
        v((2, 2 * TOK, RANK), BF), v((2 * TOK, 2 * HF), BF), v((2 * TOK, HF), BF),
        v((3, RANK, HF), BF), v((NP, *part), BF),
        v((TOK, D), F32), v((TOK, D), F32), v((TOK, D), BF),
        v(part, BF), v((3, *part), BF), v(part, BF), v((3, *part), BF),
        v((1, HF), F32), v((1, HF), F32), v((NP, 1, HF), F32),
        v((8, HF), F32), v((NP, 8, HF), F32), v((8, 8, HF), F32),
        v((3, RANK, HF), BF), v((3, ROWS, HF), F32), v((3, ROWS, HF), F32),
        v((3, 8, FF), F32), v((3, 8, FF), F32),
        dma((12,)), dma((NSEND,)), dma((2, NZ)), dma((2, 3, NZ)), dma((10,)),
        dma((NZ,)), dma((NP,)), dma((3,)), dma((3,)), dma((NP,)), dma((NP,)), dma((NP,)),
    ]
    return pl.pallas_call(
        kernel,
        out_shape=(
            jax.ShapeDtypeStruct((TOK, D), BF),
            jax.ShapeDtypeStruct((3, 8, FF), F32),
            jax.ShapeDtypeStruct((3, 8, FF), F32),
            jax.ShapeDtypeStruct((3, ROWS, FF), F32),
        ),
        in_specs=[anywhere] * 8,
        out_specs=(anywhere,) * 4,
        scratch_shapes=scratch,
        compiler_params=pltpu.CompilerParams(
            collective_id=0, has_side_effects=True, vmem_limit_bytes=60 * 1024 * 1024
        ),
    )(tokens, cotangent, w_gate, w_up, w_down, basis, first_moment, second_moment)


def solution(mesh):
    both = ("group", "member")
    placed = (
        P(both, None), P(both, None), P("member", None), P("member", None), P("member", None),
        P("member", None), P(None, "member", None), P(None, "member", None),
    )
    return jax.shard_map(
        local,
        mesh=mesh,
        in_specs=placed,
        out_specs=(P(both, None), P(None, "member", None), P(None, "member", None), P(None, "member", None)),
        check_vma=False,
    )
```

```python
import functools
import math

import jax
import jax.numpy as jnp
from jax import lax
from jax.experimental import pallas as pl
from jax.experimental.pallas import tpu as pltpu
from jax.sharding import PartitionSpec as P

BF = jnp.bfloat16
F32 = jnp.float32
MESH = pl.DeviceIdType.MESH

D = 2048
FF = 512
RANK = 256
TOK = 128
NX, NY, NZ = 4, 4, 16
NP = NX * NY
HF = FF // 2
HR = RANK // 2
ROWS = 64
PW = 3 * HF + HR
EPS_LIMIT = math.sqrt(3.0 * RANK * FF)

G0, U0, B0, D0 = 0, HF, 2 * HF, 2 * HF + HR


class Sems:
    def __init__(self, ref, count):
        self.ref, self.count, self.used = ref, count, 0

    def take(self):
        self.used += 1
        assert self.used <= self.count
        return self.ref.at[self.used - 1]


NSEND = 240

PLAN = {0: (2, 1), 2: (4, 3), 4: (6, 5), 6: (8, 7)}
DIRECT = (7, 8)


def kernel(
    tok_hbm, cot_hbm, wg_hbm, wu_hbm, wd_hbm, bas_hbm, fm_hbm, sm_hbm,
    dx_hbm, nf_hbm, ns_hbm, up_hbm,
    toks, cots, wbuf, wgv, wuv, wdv, basv, fmv, smv,
    pk, bp, msend, mrecv, mbuf,
    accx, accy, xpb, dgu, hid, lsend, lrecv,
    dxp, dxr, dxo, t0b, nearb, t1b, farb,
    sqo, sqp, sqb, lrow, lall, loth, sbuf, uov, ucv, nfv, nsv,
    lsem, ssem, zsem, xysem, psem, msem, rsem, nsem, fsem, qsem, rowsem, stsem,
):
    g = lax.axis_index("group")
    m = lax.axis_index("member")
    y, x = lax.div(g, NX), lax.rem(g, NX)
    z, c = lax.div(m, 2), lax.rem(m, 2)
    o = 1 - c
    p = g

    def dev(dx=0, dy=0, dz=0):
        yy = lax.rem(y + dy + NY, NY)
        xx = lax.rem(x + dx + NX, NX)
        zz = lax.rem(z + dz + NZ, NZ)
        return (yy * NX + xx, zz * 2 + c)

    partner = (g, z * 2 + o)

    local = []

    def load(src, dst):
        cp = pltpu.make_async_copy(src, dst, lsem.at[len(local)])
        cp.start()
        local.append(cp)
        return cp

    ld_w = [load(wg_hbm, wgv), load(wu_hbm, wuv), load(wd_hbm, wdv), load(bas_hbm, basv)]
    ld_t = [load(tok_hbm, toks.at[c]), load(cot_hbm, cots.at[c])]
    ld_m = [load(fm_hbm, fmv), load(sm_hbm, smv)]

    barrier = pltpu.get_barrier_semaphore()
    near = [partner]
    near += [dev(dz=e * t) for t in PLAN[0] for e in (1, -1)]
    near += [dev(dx=1), dev(dx=-1), dev(dx=2)]
    near += [dev(dy=1), dev(dy=-1), dev(dy=2)]
    for d in near:
        pl.semaphore_signal(barrier, inc=1, device_id=d, device_id_type=MESH)

    sends = []
    takes = Sems(ssem, NSEND)

    def remote(src, dst, rsem_, d):
        cp = pltpu.make_async_remote_copy(
            src_ref=src, dst_ref=dst, send_sem=takes.take(), recv_sem=rsem_,
            device_id=d, device_id_type=MESH,
        )
        cp.start()
        sends.append(cp)
        return cp

    def arrived(dst, rsem_):
        pltpu.make_async_remote_copy(
            src_ref=dst, dst_ref=dst, send_sem=ssem.at[0], recv_sem=rsem_,
            device_id=partner, device_id_type=MESH,
        ).wait_recv()

    for cp in ld_w:
        cp.wait()
    pr = lax.broadcasted_iota(jnp.int32, (RANK, RANK), 0)
    pc = lax.broadcasted_iota(jnp.int32, (RANK, RANK), 1)
    perm = (pr == (pc & (NZ - 1)) * NP + (pc >> 4)).astype(F32).astype(BF)
    bas = basv[...]
    bh = bas.astype(BF)
    bl = (bas - bh.astype(F32)).astype(BF)
    bp[c, 0] = jnp.dot(bh, perm, preferred_element_type=F32).astype(BF)
    bp[c, 1] = jnp.dot(bl, perm, preferred_element_type=F32).astype(BF)

    def al(v, n):
        return pl.multiple_of(v, n)

    own_rows = pl.ds(al(c * ROWS, ROWS), ROWS)
    for half, put in ((o, "partner"), (c, "own")):
        fs = pl.ds(al(half * HF, HF), HF)
        rs = pl.ds(al(half * HR, HR), HR)
        for col, width, val in (
            (G0, HF, wgv[:, fs]), (U0, HF, wuv[:, fs]), (B0, HR, bp[c, 0, :, rs]), (D0, HF, wdv[:, fs]),
        ):
            if put == "partner":
                pk[:, col : col + width] = val
            else:
                wbuf[z, own_rows, col : col + width] = val

    pl.semaphore_wait(barrier, len(near))

    remote(pk, wbuf.at[z, own_rows], psem.at[0], partner)

    def roff(h, dx=0, dy=0):
        if h == 0:
            return al(16 * lax.rem(x + dx + NX, NX), 16)
        return al(64 + 16 * lax.rem(y + dy + NY, NY), 16)

    def zchunk(zo, row):
        return wbuf.at[zo, pl.ds(row, 16)]

    def zsend(zo, h, row, dz, rel):
        remote(zchunk(zo, row), zchunk(zo, row), zsem.at[h, rel], dev(dz=dz))

    own_off = al((1 - c) * (16 * x) + c * (64 + 16 * y), 16)
    oth_off = al(c * (16 * x) + (1 - c) * (64 + 16 * y), 16)
    for h, off in ((c, own_off), (o, oth_off)):
        if h is o:
            arrived(wbuf.at[z, pl.ds(al(o * ROWS, ROWS), ROWS)], psem.at[0])
        for t in PLAN[0]:
            zsend(z, h, off, t, t)
            zsend(z, h, off, -t, NZ - t)

    for cp in ld_t:
        cp.wait()
    remote(toks.at[c], toks.at[c], psem.at[1], partner)
    remote(cots.at[c], cots.at[c], psem.at[2], partner)
    remote(bp.at[c], bp.at[c], psem.at[3], partner)

    for cp in ld_m:
        cp.wait()
    prow = lax.rem(p, 8)
    pcore = lax.div(p, 8)
    zero = jnp.zeros((2, HF), F32)
    msend[6:8, :] = zero
    mbuf[z, 6:8, :] = zero
    for i, mv in enumerate((fmv, smv)):
        for k in range(3):
            msend[3 * i + k : 3 * i + k + 1, :] = mv[k, pl.ds(prow, 1), pl.ds(al(o * HF, HF), HF)]
            mbuf[z, 3 * i + k : 3 * i + k + 1, :] = mv[k, pl.ds(prow, 1), pl.ds(al(c * HF, HF), HF)]
    remote(msend, mrecv, psem.at[4], partner)

    def origin(rel):
        return lax.rem(z - rel + NZ, NZ)

    def z_arrive(s):
        for d in (0, 1):
            rel = s if d == 0 else NZ - s
            zo = origin(rel)
            sgn = 1 if d == 0 else -1
            hs = (0, 1) if s < 8 else (d,)
            later = PLAN.get(s, ())
            for h in hs:
                arrived(zchunk(zo, roff(h)), zsem.at[h, rel])
                for t in later[:1]:
                    if t < 8 or h == d:
                        zsend(zo, h, roff(h), sgn * (t - s), (rel + sgn * (t - s)) % NZ)
            for h in hs:
                for t in later[1:]:
                    if t < 8 or h == d:
                        zsend(zo, h, roff(h), sgn * (t - s), (rel + sgn * (t - s)) % NZ)
            for h in hs:
                for e in (2, 1, -1) if s in DIRECT else (1, -1):
                    t = dev(dx=e) if h == 0 else dev(dy=e)
                    way = {1: 0, -1: 1, 2: 2}[e]
                    remote(zchunk(zo, roff(h)), zchunk(zo, roff(h)), xysem.at[h, way, rel], t)

    def pieces(s):
        if s == 8:
            return [(8, (0, 1))]
        return [(s, (0, 0)), (NZ - s, (1, 1))]

    def step_of(h, e):
        return roff(h, dx=e) if h == 0 else roff(h, dy=e)

    def xy_direct(s):
        for rel, ways in pieces(s):
            zo = origin(rel)
            for h in (0, 1):
                way = ways[h]
                e = -1 if way == 0 else 1
                ch = zchunk(zo, step_of(h, e))
                arrived(ch, xysem.at[h, way, rel])
                if s not in DIRECT:
                    t = dev(dx=-e) if h == 0 else dev(dy=-e)
                    remote(ch, ch, xysem.at[h, 2, rel], t)

    def xy_rest(s):
        for rel, ways in pieces(s):
            zo = origin(rel)
            for h in (0, 1):
                way = 1 - ways[h]
                e = -1 if way == 0 else 1
                arrived(zchunk(zo, step_of(h, e)), xysem.at[h, way, rel])
                arrived(zchunk(zo, step_of(h, 2)), xysem.at[h, 2, rel])

    def multiply(rel, first=False):
        zo = origin(rel)
        cols = pl.ds(al(zo * 128, 128), 128)
        tk = toks[:, :, cols].reshape(2 * TOK, 128)
        ck = cots[:, :, cols].reshape(2 * TOK, 128)
        ax = jnp.dot(tk, wbuf[zo, :, 0:D0], preferred_element_type=F32)
        ay = jnp.dot(ck, wbuf[zo, :, B0:PW], preferred_element_type=F32)
        if first:
            accx[...] = ax
            accy[...] = ay
        else:
            accx[...] += ax
            accy[...] += ay

    def finish(s):
        xy_rest(s)
        for rel, _ in pieces(s):
            multiply(rel)

    for s in range(1, 9):
        z_arrive(s)
        if s == 8:
            arrived(mrecv, psem.at[4])
            mine = pcore == c
            mbuf[z] = jnp.where(mine, mbuf[z], mrecv[...])
            for dz in range(1, NZ):
                remote(mbuf.at[z], mbuf.at[z], msem.at[dz], dev(dz=dz))
        if s > 1:
            xy_direct(s - 1)
        if s == 2:
            other = 1 - c
            arrived(toks.at[other], psem.at[1])
            arrived(cots.at[other], psem.at[2])
            multiply(0, first=True)
        if s > 3:
            finish(s - 3)
    xy_direct(8)
    for s in (6, 7, 8):
        finish(s)

    hc = pl.ds(al(c * HR, HR), HR)
    ho = pl.ds(al(o * HR, HR), HR)
    xpb[0, :, hc] = accx[:, B0 : B0 + HR].astype(BF)
    xpb[1, :, hc] = accy[:, 0:HR].astype(BF)
    remote(xpb.at[:, :, hc], xpb.at[:, :, hc], psem.at[5], partner)
    gate = accx[:, G0 : G0 + HF]
    up = accx[:, U0 : U0 + HF]
    dhid = accy[:, HR : HR + HF]
    sig = jax.nn.sigmoid(gate)
    silu = gate * sig
    hid[...] = (silu * up).astype(BF)
    dgu[:, 0:HF] = (dhid * up * sig * (1.0 + gate * (1.0 - sig))).astype(BF)
    dgu[:, HF : 2 * HF] = (dhid * silu).astype(BF)
    arrived(xpb.at[:, :, ho], psem.at[5])

    over_rows = (((0,), (0,)), ((), ()))
    l01 = lax.dot_general(xpb[0], dgu[...], over_rows, preferred_element_type=F32)
    lsend[0] = l01[:, 0:HF].astype(BF)
    lsend[1] = l01[:, HF : 2 * HF].astype(BF)
    lsend[2] = lax.dot_general(xpb[1], hid[...], over_rows, preferred_element_type=F32).astype(BF)

    plane = [(dx, dy) for dy in range(NY) for dx in range(NX) if (dx, dy) != (0, 0)]
    far_first = sorted(plane, key=lambda t: -(min(t[0], NX - t[0]) + min(t[1], NY - t[1])))

    def back(dx, dy):
        return ((-dy) % NY) * NX + (-dx) % NX

    def part_of(dx, dy):
        return lax.rem(y + dy, NY) * NX + lax.rem(x + dx, NX)

    def rows_of(q):
        return pl.ds(al(q * NZ, NZ), NZ)

    for dx, dy in far_first:
        q = part_of(dx, dy)
        remote(lsend.at[:, rows_of(q)], lrecv.at[p], rsem.at[back(dx, dy)], dev(dx=dx, dy=dy))
    lrecv[p] = lsend[:, rows_of(p)]

    def dx_of(core, out):
        rows = pl.ds(al(core * TOK, TOK), TOK)
        lhs = dgu[rows, :]

        @pl.loop(0, NZ)
        def _(i):
            out[:, pl.ds(al(i * 128, 128), 128)] = lax.dot_general(
                lhs, wbuf[i, :, 0 : 2 * HF], (((1,), (1,)), ((), ())), preferred_element_type=F32
            )

    dx_of(o, dxp)
    remote(dxp, dxr, psem.at[6], partner)

    def sum_parts(own, bufs):
        total = own
        for b in bufs:
            total = total + b.astype(F32)
        return total

    for dx, dy in plane:
        arrived(lrecv.at[part_of(dx, dy)], rsem.at[dy * NX + dx])
    total = lrecv[0].astype(F32)
    for q in range(1, NP):
        total = total + lrecv[q].astype(F32)
    t0b[...] = total.astype(BF)
    for i, dz in enumerate((1, -1, -2)):
        remote(t0b, nearb.at[i], nsem.at[i], dev(dz=dz))
    for i in range(3):
        arrived(nearb.at[i], nsem.at[i])
    total = sum_parts(total, [nearb[i] for i in range(3)])
    t1b[...] = total.astype(BF)
    for i, dz in ((2, 8), (0, 4), (1, -4)):
        remote(t1b, farb.at[i], fsem.at[i], dev(dz=dz))

    rows = pl.ds(al(c * TOK, TOK), TOK)
    arrived(dxr, psem.at[6])
    lhs_own = dgu[rows, :]

    @pl.loop(0, NZ)
    def _(i):
        cols = pl.ds(al(i * 128, 128), 128)
        part = lax.dot_general(
            lhs_own, wbuf[i, :, 0 : 2 * HF], (((1,), (1,)), ((), ())), preferred_element_type=F32
        )
        dxo[:, cols] = (part + dxr[:, cols]).astype(BF)

    outs = []

    def store(src, dst):
        cp = pltpu.make_async_copy(src, dst, lsem.at[8 + len(outs)])
        cp.start()
        outs.append(cp)

    store(dxo, dx_hbm)

    for i in range(3):
        arrived(farb.at[i], fsem.at[i])
    total = sum_parts(total, [farb[i] for i in range(3)])

    sq = jnp.sum(jnp.sum(total * total, axis=0), axis=0, keepdims=True)
    sq = jnp.sum(sq, axis=1, keepdims=True)
    sqo[...] = jnp.broadcast_to(sq, (1, HF))
    remote(sqo, sqp, psem.at[7], partner)
    zrow = lax.broadcasted_iota(jnp.int32, (3, NZ, HF), 1) == z
    mine3 = jnp.sum(jnp.where(zrow, total, 0.0), axis=1)
    lrow[0:3, :] = mine3
    lrow[3:8, :] = jnp.zeros((5, HF), F32)
    arrived(sqp, psem.at[7])
    sqb[p] = sqo[...] + sqp[...]
    for dx, dy in far_first:
        remote(sqb.at[p], sqb.at[p], qsem.at[back(dx, dy)], dev(dx=dx, dy=dy))
    lall[p] = lrow[...]
    for dx, dy in far_first:
        remote(lrow, lall.at[p], rowsem.at[back(dx, dy)], dev(dx=dx, dy=dy))
    for dz in range(1, NZ):
        arrived(mbuf.at[origin(dz)], msem.at[dz])
    for dx, dy in plane:
        arrived(sqb.at[part_of(dx, dy)], qsem.at[dy * NX + dx])
    ssum = sqb[0]
    for q in range(1, NP):
        ssum = ssum + sqb[q]
    factor = jnp.minimum(1.0, EPS_LIMIT / jnp.sqrt(ssum + 1e-06))

    def adam(low, first, second):
        grad = factor * low
        nf = 0.5 * first + 0.5 * grad
        ns = 0.9 * second + 0.1 * grad * grad
        return nf, ns

    for k in range(3):
        nf, ns = adam(total[k], mbuf[:, k, :], mbuf[:, 3 + k, :])
        sbuf[k, rows_of(p), :] = (nf / (jnp.sqrt(ns) + 1e-08)).astype(BF)
    for dx, dy in far_first:
        mine = sbuf.at[:, rows_of(p)]
        remote(mine, mine, stsem.at[back(dx, dy)], dev(dx=dx, dy=dy))

    for dx, dy in plane:
        arrived(lall.at[part_of(dx, dy)], rowsem.at[dy * NX + dx])
    remote(lall.at[pl.ds(al(o * 8, 8), 8)], loth, psem.at[8], partner)
    fc = pl.ds(al(c * HF, HF), HF)
    fo = pl.ds(al(o * HF, HF), HF)
    for k in range(3):
        nf, ns = adam(lall[pl.ds(al(c * 8, 8), 8), k, :], fmv[k, :, fc], smv[k, :, fc])
        nfv[k, :, fc] = nf
        nsv[k, :, fc] = ns
    arrived(loth, psem.at[8])
    for k in range(3):
        nf, ns = adam(loth[:, k, :], fmv[k, :, fo], smv[k, :, fo])
        nfv[k, :, fo] = nf
        nsv[k, :, fo] = ns
    store(nfv, nf_hbm)
    store(nsv, ns_hbm)

    arrived(bp.at[o], psem.at[3])
    for dx, dy in plane:
        arrived(sbuf.at[:, rows_of(part_of(dx, dy))], stsem.at[dy * NX + dx])

    def update(core, k):
        st = sbuf[k]
        return jnp.dot(bp[core, 0], st, preferred_element_type=F32) + jnp.dot(
            bp[core, 1], st, preferred_element_type=F32
        )

    for k in range(3):
        uov[k] = update(o, k)
    remote(uov, up_hbm.at[:, :, fc], psem.at[9], partner)
    for k in range(3):
        ucv[k] = update(c, k)
    store(ucv, up_hbm.at[:, :, fc])
    arrived(up_hbm.at[:, :, fo], psem.at[9])
    for cp in outs:
        cp.wait()
    for cp in sends:
        cp.wait_send()


def local(tokens, cotangent, w_gate, w_up, w_down, basis, first_moment, second_moment):
    anywhere = pl.BlockSpec(memory_space=pl.ANY)
    dma = pltpu.SemaphoreType.DMA
    v = pltpu.VMEM
    part = (3, NZ, HF)
    scratch = [
        v((2, TOK, D), BF), v((2, TOK, D), BF), v((NZ, 128, PW), BF),
        v((ROWS, FF), BF), v((ROWS, FF), BF), v((ROWS, FF), BF), v((ROWS, RANK), F32),
        v((3, 8, FF), F32), v((3, 8, FF), F32),
        v((ROWS, PW), BF), v((2, 2, ROWS, RANK), BF),
        v((8, HF), F32), v((8, HF), F32), v((NZ, 8, HF), F32),
        v((2 * TOK, D0), F32), v((2 * TOK, HR + HF), F32),
        v((2, 2 * TOK, RANK), BF), v((2 * TOK, 2 * HF), BF), v((2 * TOK, HF), BF),
        v((3, RANK, HF), BF), v((NP, *part), BF),
        v((TOK, D), F32), v((TOK, D), F32), v((TOK, D), BF),
        v(part, BF), v((3, *part), BF), v(part, BF), v((3, *part), BF),
        v((1, HF), F32), v((1, HF), F32), v((NP, 1, HF), F32),
        v((8, HF), F32), v((NP, 8, HF), F32), v((8, 8, HF), F32),
        v((3, RANK, HF), BF), v((3, ROWS, HF), F32), v((3, ROWS, HF), F32),
        v((3, 8, FF), F32), v((3, 8, FF), F32),
        dma((12,)), dma((NSEND,)), dma((2, NZ)), dma((2, 3, NZ)), dma((10,)),
        dma((NZ,)), dma((NP,)), dma((3,)), dma((3,)), dma((NP,)), dma((NP,)), dma((NP,)),
    ]
    return pl.pallas_call(
        kernel,
        out_shape=(
            jax.ShapeDtypeStruct((TOK, D), BF),
            jax.ShapeDtypeStruct((3, 8, FF), F32),
            jax.ShapeDtypeStruct((3, 8, FF), F32),
            jax.ShapeDtypeStruct((3, ROWS, FF), F32),
        ),
        in_specs=[anywhere] * 8,
        out_specs=(anywhere,) * 4,
        scratch_shapes=scratch,
        compiler_params=pltpu.CompilerParams(
            collective_id=0, has_side_effects=True, vmem_limit_bytes=60 * 1024 * 1024
        ),
    )(tokens, cotangent, w_gate, w_up, w_down, basis, first_moment, second_moment)


def solution(mesh):
    both = ("group", "member")
    placed = (
        P(both, None), P(both, None), P("member", None), P("member", None), P("member", None),
        P("member", None), P(None, "member", None), P(None, "member", None),
    )
    return jax.shard_map(
        local,
        mesh=mesh,
        in_specs=placed,
        out_specs=(P(both, None), P(None, "member", None), P(None, "member", None), P(None, "member", None)),
        check_vma=False,
    )
```

```python
import functools
import math

import jax
import jax.numpy as jnp
from jax import lax
from jax.experimental import pallas as pl
from jax.experimental.pallas import tpu as pltpu
from jax.sharding import PartitionSpec as P

BF = jnp.bfloat16
F32 = jnp.float32
MESH = pl.DeviceIdType.MESH

D = 2048
FF = 512
RANK = 256
TOK = 128
NX, NY, NZ = 4, 4, 16
NP = NX * NY
HF = FF // 2
HR = RANK // 2
ROWS = 64
PW = 3 * HF + HR
EPS_LIMIT = math.sqrt(3.0 * RANK * FF)

G0, U0, B0, D0 = 0, HF, 2 * HF, 2 * HF + HR


class Pool:
    def __init__(self, ref, count, near):
        self.ref, self.count, self.near, self.started, self.done = ref, count, near, [], 0

    def start(self, src, dst, recv, device, like=None):
        if len(self.started) - self.done == self.count:
            self.wait_oldest(recv)
        pltpu.make_async_remote_copy(
            src_ref=src, dst_ref=dst, send_sem=self.ref.at[len(self.started) % self.count],
            recv_sem=recv, device_id=device, device_id_type=MESH,
        ).start()
        self.started.append(src if like is None else like)

    def wait_oldest(self, recv):
        like = self.started[self.done]
        like = like() if callable(like) else like
        pltpu.make_async_remote_copy(
            src_ref=like, dst_ref=like, send_sem=self.ref.at[self.done % self.count],
            recv_sem=recv, device_id=self.near, device_id_type=MESH,
        ).wait_send()
        self.done += 1

    def drain(self):
        while self.done < len(self.started):
            self.wait_oldest(self.ref.at[0])


NLEAD, NBOTH, NHELP, NGATHER = 72, 24, 8, 160

PLAN = {0: (2, 1), 2: (4, 3), 4: (6, 5), 6: (8, 7)}
DIRECT = (7, 8)


def kernel(
    tok_hbm, cot_hbm, wg_hbm, wu_hbm, wd_hbm, bas_hbm, fm_hbm, sm_hbm,
    dxo, nfv, nsv, upv,
    toks, cots, wbuf, wgv, wuv, wdv, basv, fmv, smv,
    pk, bp, msend, mrecv, mbuf,
    accx, accy, xpb, dgu, hid, lsend, lrecv,
    dxp, dxr, tv, t0b, nearb, t1b, farb,
    sqb, sfac, lrow, lall, loth, sbuf, uov,
    lsem, lead_sem, both_sem, help_sem, gather_sem, zsem, xysem, psem, msem, rsem, nsem, fsem, qsem, rowsem, stsem,
):
    g = lax.axis_index("group")
    m = lax.axis_index("member")
    y, x = lax.div(g, NX), lax.rem(g, NX)
    z, c = lax.div(m, 2), lax.rem(m, 2)
    o = 1 - c
    p = g
    leads, helps = c == 1, c == 0

    xs = [x] + [lax.rem(x + d, NX) for d in range(1, NX)]
    ys = [y] + [lax.rem(y + d, NY) for d in range(1, NY)]
    zs = [z] + [lax.rem(z + d, NZ) for d in range(1, NZ)]
    groups = {(i, j): ys[j] * NX + xs[i] for i in range(NX) for j in range(NY)}
    groups[0, 0] = g
    members = [zs[i] * 2 + c for i in range(NZ)]
    leaders = [zs[i] * 2 + 1 for i in range(NZ)]
    xrows = [16 * xs[i] for i in range(NX)]
    yrows = [64 + 16 * ys[i] for i in range(NY)]

    def dev(dx=0, dy=0, dz=0, lead=False):
        return (groups[dx % NX, dy % NY], (leaders if lead else members)[dz % NZ])

    partner = (g, z * 2 + o)

    local = []

    def load(src, dst):
        cp = pltpu.make_async_copy(src, dst, lsem.at[len(local)])
        cp.start()
        local.append(cp)
        return cp

    ld_w = [load(wg_hbm, wgv), load(wu_hbm, wuv), load(wd_hbm, wdv), load(bas_hbm, basv)]
    ld_t = [load(tok_hbm, toks.at[c]), load(cot_hbm, cots.at[c])]
    ld_m = [load(fm_hbm, fmv), load(sm_hbm, smv)]

    barrier = pltpu.get_barrier_semaphore()
    near = [partner, dev(dx=1), dev(dx=-1), dev(dx=2), dev(dy=1), dev(dy=-1), dev(dy=2)]
    near += [dev(dz=e * t) for t in PLAN[0] for e in (1, -1)]

    for d in near:
        pl.semaphore_signal(barrier, inc=1, device_id=d, device_id_type=MESH)

    lead = Pool(lead_sem, NLEAD, partner)
    both = Pool(both_sem, NBOTH, partner)
    helper = Pool(help_sem, NHELP, partner)
    gather = Pool(gather_sem, NGATHER, partner)

    def chunk():
        return wbuf.at[0, pl.ds(0, 16)]

    def part():
        return lsend.at[:, pl.ds(0, NZ)]


    def arrived(dst, recv):
        pltpu.make_async_remote_copy(
            src_ref=dst, dst_ref=dst, send_sem=both_sem.at[0], recv_sem=recv,
            device_id=partner, device_id_type=MESH,
        ).wait_recv()

    def al(v, n):
        return pl.multiple_of(v, n)

    def roff(h, e=0):
        return al(xrows[e % NX] if h == 0 else yrows[e % NY], 16)

    for cp in ld_w:
        cp.wait()
    pr = lax.broadcasted_iota(jnp.int32, (RANK, RANK), 0)
    pc = lax.broadcasted_iota(jnp.int32, (RANK, RANK), 1)
    perm = (pr == (pc & (NZ - 1)) * NP + (pc >> 4)).astype(F32).astype(BF)
    bas = basv[...]
    bh = bas.astype(BF)
    bl = (bas - bh.astype(F32)).astype(BF)
    bp[c, 0] = jnp.dot(bh, perm, preferred_element_type=F32).astype(BF)
    bp[c, 1] = jnp.dot(bl, perm, preferred_element_type=F32).astype(BF)
    own_rows = pl.ds(al(c * ROWS, ROWS), ROWS)
    for half, put in ((o, "partner"), (c, "own")):
        fs = pl.ds(al(half * HF, HF), HF)
        rs = pl.ds(al(half * HR, HR), HR)
        for col, width, val in (
            (G0, HF, wgv[:, fs]), (U0, HF, wuv[:, fs]), (B0, HR, bp[c, 0, :, rs]), (D0, HF, wdv[:, fs]),
        ):
            if put == "partner":
                pk[:, col : col + width] = val
            else:
                wbuf[z, own_rows, col : col + width] = val

    pl.semaphore_wait(barrier, len(near))

    both.start(pk, wbuf.at[z, own_rows], psem.at[0], partner)

    def held(zo, row):
        return wbuf.at[zo, pl.ds(row, 16)]

    def zsend(zo, h, row, dz, rel):
        gather.start(held(zo, row), held(zo, row), zsem.at[h, rel], dev(dz=dz), chunk)

    own_off = al((1 - c) * xrows[0] + c * yrows[0], 16)
    oth_off = al(c * xrows[0] + (1 - c) * yrows[0], 16)
    for h, off in ((c, own_off), (o, oth_off)):
        if h is o:
            arrived(wbuf.at[z, pl.ds(al(o * ROWS, ROWS), ROWS)], psem.at[0])
        for t in PLAN[0]:
            zsend(z, h, off, t, t)
            zsend(z, h, off, -t, NZ - t)

    for cp in ld_t:
        cp.wait()
    both.start(toks.at[c], toks.at[c], psem.at[1], partner)
    both.start(cots.at[c], cots.at[c], psem.at[2], partner)

    for cp in ld_m:
        cp.wait()
    prow = lax.rem(p, 8)
    pcore = lax.div(p, 8)
    msend[6:8, :] = jnp.zeros((2, FF), F32)
    for i, mv in enumerate((fmv, smv)):
        for k in range(3):
            msend[3 * i + k : 3 * i + k + 1, :] = mv[k, pl.ds(prow, 1), :]

    @pl.when(helps)
    def _():
        helper.start(bp.at[0], bp.at[0], psem.at[3], partner, lambda: bp.at[0])
        helper.start(msend, mrecv, psem.at[4], partner)

    def origin(rel):
        return zs[-rel % NZ]

    def aside(h, e):
        return dev(dx=e) if h == 0 else dev(dy=e)

    def z_arrive(s):
        for d in (0, 1):
            rel = s if d == 0 else NZ - s
            zo = origin(rel)
            sgn = 1 if d == 0 else -1
            hs = (0, 1) if s < 8 else (d,)
            later = PLAN.get(s, ())
            for h in hs:
                arrived(held(zo, roff(h)), zsem.at[h, rel])
                for t in later[:1]:
                    if t < 8 or h == d:
                        zsend(zo, h, roff(h), sgn * (t - s), (rel + sgn * (t - s)) % NZ)
            for h in hs:
                for t in later[1:]:
                    if t < 8 or h == d:
                        zsend(zo, h, roff(h), sgn * (t - s), (rel + sgn * (t - s)) % NZ)
            for h in hs:
                there = held(zo, roff(h))
                for e in (2, 1, -1) if s in DIRECT else (1, -1):
                    way = {1: 0, -1: 1, 2: 2}[e]
                    gather.start(there, there, xysem.at[h, way, rel], aside(h, e), chunk)

    def pieces(s):
        if s == 8:
            return [(8, (0, 1))]
        return [(s, (0, 0)), (NZ - s, (1, 1))]

    def xy_direct(s):
        for rel, ways in pieces(s):
            for h in (0, 1):
                e = -1 if ways[h] == 0 else 1
                ch = held(origin(rel), roff(h, e))
                arrived(ch, xysem.at[h, ways[h], rel])
                if s not in DIRECT:
                    gather.start(ch, ch, xysem.at[h, 2, rel], aside(h, -e), chunk)

    def xy_rest(s):
        for rel, ways in pieces(s):
            for h in (0, 1):
                way = 1 - ways[h]
                e = -1 if way == 0 else 1
                arrived(held(origin(rel), roff(h, e)), xysem.at[h, way, rel])
                arrived(held(origin(rel), roff(h, 2)), xysem.at[h, 2, rel])

    def multiply(rel, first=False):
        zo = origin(rel)
        cols = pl.ds(al(zo * 128, 128), 128)
        tk = toks[:, :, cols].reshape(2 * TOK, 128)
        ck = cots[:, :, cols].reshape(2 * TOK, 128)
        ax = jnp.dot(tk, wbuf[zo, :, 0:D0], preferred_element_type=F32)
        ay = jnp.dot(ck, wbuf[zo, :, B0:PW], preferred_element_type=F32)
        if first:
            accx[...] = ax
            accy[...] = ay
        else:
            accx[...] += ax
            accy[...] += ay

    def finish(s):
        xy_rest(s)
        for rel, _ in pieces(s):
            multiply(rel)

    for s in range(1, 9):
        z_arrive(s)
        if s > 1:
            xy_direct(s - 1)
        if s == 2:
            arrived(toks.at[o], psem.at[1])
            arrived(cots.at[o], psem.at[2])
            multiply(0, first=True)
        if s > 3:
            finish(s - 3)

    @pl.when(leads)
    def _():
        arrived(mrecv, psem.at[4])
        mbuf[z] = jnp.where(pcore == 1, msend[...], mrecv[...])
        for dz in range(1, NZ):
            lead.start(mbuf.at[z], mbuf.at[z], msem.at[dz], dev(dz=dz, lead=True), lambda: mbuf.at[0])

    xy_direct(8)
    for s in (6, 7, 8):
        finish(s)

    hc = pl.ds(al(c * HR, HR), HR)
    ho = pl.ds(al(o * HR, HR), HR)
    xpb[0, :, hc] = accx[:, B0 : B0 + HR].astype(BF)
    xpb[1, :, hc] = accy[:, 0:HR].astype(BF)
    both.start(xpb.at[:, :, hc], xpb.at[:, :, hc], psem.at[5], partner)
    gate = accx[:, G0 : G0 + HF]
    up = accx[:, U0 : U0 + HF]
    dhid = accy[:, HR : HR + HF]
    sig = jax.nn.sigmoid(gate)
    silu = gate * sig
    hid[...] = (silu * up).astype(BF)
    dgu[:, 0:HF] = (dhid * up * sig * (1.0 + gate * (1.0 - sig))).astype(BF)
    dgu[:, HF : 2 * HF] = (dhid * silu).astype(BF)
    arrived(xpb.at[:, :, ho], psem.at[5])

    over_rows = (((0,), (0,)), ((), ()))
    l01 = lax.dot_general(xpb[0], dgu[...], over_rows, preferred_element_type=F32)
    lsend[0] = l01[:, 0:HF].astype(BF)
    lsend[1] = l01[:, HF : 2 * HF].astype(BF)
    lsend[2] = lax.dot_general(xpb[1], hid[...], over_rows, preferred_element_type=F32).astype(BF)

    plane = [(dx, dy) for dy in range(NY) for dx in range(NX) if (dx, dy) != (0, 0)]
    far_first = sorted(plane, key=lambda t: -(min(t[0], NX - t[0]) + min(t[1], NY - t[1])))

    def back(dx, dy):
        return ((-dy) % NY) * NX + (-dx) % NX

    def part_of(dx, dy):
        return groups[dx, dy]

    def rows_of(q):
        return pl.ds(al(q * NZ, NZ), NZ)

    for dx, dy in far_first:
        q = part_of(dx, dy)
        both.start(lsend.at[:, rows_of(q)], lrecv.at[p, c], rsem.at[c, back(dx, dy)], dev(dx=dx, dy=dy, lead=True), part)

    @pl.when(leads)
    def _():
        lrecv[p, 1] = lsend[:, rows_of(p)]

    @pl.when(helps)
    def _():
        helper.start(lsend.at[:, rows_of(p)], lrecv.at[p, 0], rsem.at[0, 0], partner, part)

    def dx_part(core, put):
        lhs = dgu[pl.ds(al(core * TOK, TOK), TOK), :]

        @pl.loop(0, NZ)
        def _(i):
            put(pl.ds(al(i * 128, 128), 128), lax.dot_general(
                lhs, wbuf[i, :, 0 : 2 * HF], (((1,), (1,)), ((), ())), preferred_element_type=F32
            ))

    def put_partner(cols, val):
        dxp[:, cols] = val

    def put_own(cols, val):
        dxo[:, cols] = (val + dxr[:, cols]).astype(BF)

    dx_part(o, put_partner)
    both.start(dxp, dxr, psem.at[6], partner)

    @pl.when(leads)
    def _():
        for half in (0, 1):
            for dx, dy in plane:
                arrived(lrecv.at[part_of(dx, dy), half], rsem.at[half, dy * NX + dx])
        arrived(lrecv.at[p, 0], rsem.at[0, 0])
        total = lrecv[0].astype(F32)
        for q in range(1, NP):
            total = total + lrecv[q].astype(F32)
        t0b[...] = total.astype(BF)
        for i, dz in enumerate((1, -1, -2)):
            lead.start(t0b, nearb.at[i], nsem.at[i], dev(dz=dz, lead=True))
        for i in range(3):
            arrived(nearb.at[i], nsem.at[i])
        for i in range(3):
            total = total + nearb[i].astype(F32)
        t1b[...] = total.astype(BF)
        for i, dz in ((2, 8), (0, 4), (1, -4)):
            lead.start(t1b, farb.at[i], fsem.at[i], dev(dz=dz, lead=True))
        tv[...] = total

    arrived(dxr, psem.at[6])
    dx_part(c, put_own)
    def adam(low, first, second, factor):
        grad = factor * low
        nf = 0.5 * first + 0.5 * grad
        ns = 0.9 * second + 0.1 * grad * grad
        return nf, ns

    def factor_of(ssum):
        return jnp.minimum(1.0, EPS_LIMIT / jnp.sqrt(ssum + 1e-06))

    halves = (slice(0, HF), slice(HF, FF))

    def moments(low):
        factor = factor_of(sfac[0:1, :])
        for k in range(3):
            nf, ns = adam(low(k), fmv[k], smv[k], jnp.concatenate([factor, factor], axis=1))
            nfv[k] = nf
            nsv[k] = ns

    @pl.when(leads)
    def _():
        for i in range(3):
            arrived(farb.at[i], fsem.at[i])
        total = tv[...]
        for i in range(3):
            total = total + farb[i].astype(F32)
        flat = total.reshape(6 * NZ, HF)
        sq = jnp.sum(jnp.sum(flat * flat, axis=0, keepdims=True), axis=1, keepdims=True)
        sqb[p] = jnp.broadcast_to(sq, (1, HF))
        for dx, dy in far_first:
            lead.start(sqb.at[p], sqb.at[p], qsem.at[back(dx, dy)], dev(dx=dx, dy=dy, lead=True), lambda: sqb.at[0])
        zrow = lax.broadcasted_iota(jnp.int32, (3, NZ, HF), 1) == z
        lrow[3:8, :] = jnp.zeros((5, FF), F32)
        for half in (0, 1):
            lrow[0:3, halves[half]] = jnp.sum(jnp.where(zrow, total[half], 0.0), axis=1)
        lall[p] = lrow[...]
        for dx, dy in far_first:
            lead.start(lrow, lall.at[p], rowsem.at[back(dx, dy)], dev(dx=dx, dy=dy, lead=True))
        for dz in range(1, NZ):
            arrived(mbuf.at[origin(dz)], msem.at[dz])
        for dx, dy in plane:
            arrived(sqb.at[part_of(dx, dy)], qsem.at[dy * NX + dx])
        ssum = sqb[0]
        for q in range(1, NP):
            ssum = ssum + sqb[q]
        sfac[0:1, :] = ssum
        factor = factor_of(ssum)
        for k in range(3):
            for half in (0, 1):
                nf, ns = adam(total[half, k], mbuf[:, k, halves[half]], mbuf[:, 3 + k, halves[half]], factor)
                sbuf[k, rows_of(p), halves[half]] = (nf / (jnp.sqrt(ns) + 1e-08)).astype(BF)
        mine = sbuf.at[:, rows_of(p)]
        for dx, dy in far_first:
            lead.start(mine, mine, stsem.at[back(dx, dy)], dev(dx=dx, dy=dy, lead=True), lambda: sbuf.at[:, pl.ds(0, NZ)])
        for dx, dy in plane:
            arrived(lall.at[part_of(dx, dy)], rowsem.at[dy * NX + dx])
        lead.start(sfac, sfac, psem.at[8], partner)
        lead.start(lall.at[0:8], loth, psem.at[10], partner, lambda: lall.at[0:8])
        moments(lambda k: lall[8:16, k, :])

    @pl.when(helps)
    def _():
        arrived(sfac, psem.at[8])
        arrived(loth, psem.at[10])
        moments(lambda k: loth[:, k, :])

    def update(core, k):
        st = sbuf[k]
        return jnp.dot(bp[core, 0], st, preferred_element_type=F32) + jnp.dot(
            bp[core, 1], st, preferred_element_type=F32
        )

    @pl.when(leads)
    def _():
        arrived(bp.at[0], psem.at[3])
        for dx, dy in plane:
            arrived(sbuf.at[:, rows_of(part_of(dx, dy))], stsem.at[dy * NX + dx])
        for k in range(3):
            uov[k] = update(0, k)
        lead.start(uov, upv, psem.at[9], partner)
        for k in range(3):
            upv[k] = update(1, k)
        lead.drain()

    @pl.when(helps)
    def _():
        arrived(upv, psem.at[9])
        helper.drain()

    both.drain()
    gather.drain()


def local(tokens, cotangent, w_gate, w_up, w_down, basis, first_moment, second_moment):
    anywhere = pl.BlockSpec(memory_space=pl.ANY)
    dma = pltpu.SemaphoreType.DMA
    v = pltpu.VMEM
    part = (2, 3, NZ, HF)
    scratch = [
        v((2, TOK, D), BF), v((2, TOK, D), BF), v((NZ, 128, PW), BF),
        v((ROWS, FF), BF), v((ROWS, FF), BF), v((ROWS, FF), BF), v((ROWS, RANK), F32),
        v((3, 8, FF), F32), v((3, 8, FF), F32),
        v((ROWS, PW), BF), v((2, 2, ROWS, RANK), BF),
        v((8, FF), F32), v((8, FF), F32), v((NZ, 8, FF), F32),
        v((2 * TOK, D0), F32), v((2 * TOK, HR + HF), F32),
        v((2, 2 * TOK, RANK), BF), v((2 * TOK, 2 * HF), BF), v((2 * TOK, HF), BF),
        v((3, RANK, HF), BF), v((NP, *part), BF),
        v((TOK, D), F32), v((TOK, D), F32),
        v(part, F32), v(part, BF), v((3, *part), BF), v(part, BF), v((3, *part), BF),
        v((NP, 1, HF), F32), v((8, HF), F32),
        v((8, FF), F32), v((NP, 8, FF), F32), v((8, 8, FF), F32),
        v((3, RANK, FF), BF), v((3, ROWS, FF), F32),
        dma((8,)), dma((NLEAD,)), dma((NBOTH,)), dma((NHELP,)), dma((NGATHER,)), dma((2, NZ)), dma((2, 3, NZ)), dma((11,)),
        dma((NZ,)), dma((2, NP)), dma((3,)), dma((3,)), dma((NP,)), dma((NP,)), dma((NP,)),
    ]
    kept = [((TOK, D), BF), ((3, 8, FF), F32), ((3, 8, FF), F32), ((3, ROWS, FF), F32)]
    inside = pl.BlockSpec(memory_space=pltpu.VMEM)
    results = pl.pallas_call(
        kernel,
        out_shape=tuple(pltpu.VMEM(*k) for k in kept),
        in_specs=[anywhere] * 8,
        out_specs=(inside,) * 4,
        scratch_shapes=scratch,
        compiler_params=pltpu.CompilerParams(
            collective_id=0, has_side_effects=True, vmem_limit_bytes=58 * 1024 * 1024
        ),
    )(tokens, cotangent, w_gate, w_up, w_down, basis, first_moment, second_moment)
    return pl.pallas_call(
        put_out,
        out_shape=tuple(jax.ShapeDtypeStruct(*k) for k in kept),
        in_specs=[inside] * 4,
        out_specs=(anywhere,) * 4,
        scratch_shapes=[dma((4,))],
        compiler_params=pltpu.CompilerParams(vmem_limit_bytes=4 * 1024 * 1024),
    )(*results)


def put_out(a, b, c, d, a_hbm, b_hbm, c_hbm, d_hbm, sem):
    pairs = ((a, a_hbm), (b, b_hbm), (c, c_hbm), (d, d_hbm))
    copies = [pltpu.make_async_copy(src, dst, sem.at[i]) for i, (src, dst) in enumerate(pairs)]
    for cp in copies:
        cp.start()
    for cp in copies:
        cp.wait()


def solution(mesh):
    both = ("group", "member")
    placed = (
        P(both, None), P(both, None), P("member", None), P("member", None), P("member", None),
        P("member", None), P(None, "member", None), P(None, "member", None),
    )
    return jax.shard_map(
        local,
        mesh=mesh,
        in_specs=placed,
        out_specs=(P(both, None), P(None, "member", None), P(None, "member", None), P(None, "member", None)),
        check_vma=False,
    )
```

```python
import functools
import math

import jax
import jax.numpy as jnp
from jax import lax
from jax.experimental import pallas as pl
from jax.experimental.pallas import tpu as pltpu
from jax.sharding import PartitionSpec as P

BF = jnp.bfloat16
F32 = jnp.float32
MESH = pl.DeviceIdType.MESH

D = 2048
FF = 512
RANK = 256
TOK = 128
NX, NY, NZ = 4, 4, 16
NP = NX * NY
HF = FF // 2
HR = RANK // 2
ROWS = 64
PW = 3 * HF + HR
EPS_LIMIT = math.sqrt(3.0 * RANK * FF)

G0, U0, B0, D0 = 0, HF, 2 * HF, 2 * HF + HR


class Pool:
    def __init__(self, ref, count, near):
        self.ref, self.count, self.near, self.started, self.done = ref, count, near, [], 0

    def start(self, src, dst, recv, device, like=None):
        if len(self.started) - self.done == self.count:
            self.wait_oldest(recv)
        pltpu.make_async_remote_copy(
            src_ref=src, dst_ref=dst, send_sem=self.ref.at[len(self.started) % self.count],
            recv_sem=recv, device_id=device, device_id_type=MESH,
        ).start()
        self.started.append(src if like is None else like)

    def wait_oldest(self, recv):
        like = self.started[self.done]
        like = like() if callable(like) else like
        pltpu.make_async_remote_copy(
            src_ref=like, dst_ref=like, send_sem=self.ref.at[self.done % self.count],
            recv_sem=recv, device_id=self.near, device_id_type=MESH,
        ).wait_send()
        self.done += 1

    def drain(self):
        while self.done < len(self.started):
            self.wait_oldest(self.ref.at[0])


NLEAD, NBOTH, NHELP, NGATHER = 72, 24, 8, 160

PLAN = {0: (2, 1), 2: (4, 3), 4: (6, 5), 6: (8, 7)}
DIRECT = (7, 8)


def kernel(
    tok_hbm, cot_hbm, wg_hbm, wu_hbm, wd_hbm, bas_hbm, fm_hbm, sm_hbm,
    dxo, nfv, nsv, upv,
    toks, cots, wbuf, wgv, wuv, wdv, basv, fmv, smv,
    pk, bp, msend, mrecv, mbuf,
    accx, accy, xpb, dgu, hid, lsend, lrecv,
    dxp, dxr, tv, t0b, nearb, t1b, farb,
    sqb, sfac, lrow, lall, loth, sbuf, uov,
    lsem, lead_sem, both_sem, help_sem, gather_sem, part_sem, zsem, xysem, psem, msem, rsem, nsem, fsem, qsem, rowsem, stsem,
):
    g = lax.axis_index("group")
    m = lax.axis_index("member")
    y, x = lax.div(g, NX), lax.rem(g, NX)
    z, c = lax.div(m, 2), lax.rem(m, 2)
    o = 1 - c
    p = g
    leads, helps = c == 1, c == 0

    xs = [x] + [lax.rem(x + d, NX) for d in range(1, NX)]
    ys = [y] + [lax.rem(y + d, NY) for d in range(1, NY)]
    zs = [z] + [lax.rem(z + d, NZ) for d in range(1, NZ)]
    groups = {(i, j): ys[j] * NX + xs[i] for i in range(NX) for j in range(NY)}
    groups[0, 0] = g
    members = [zs[i] * 2 + c for i in range(NZ)]
    leaders = [zs[i] * 2 + 1 for i in range(NZ)]
    xrows = [16 * xs[i] for i in range(NX)]
    yrows = [64 + 16 * ys[i] for i in range(NY)]

    def dev(dx=0, dy=0, dz=0, lead=False):
        return (groups[dx % NX, dy % NY], (leaders if lead else members)[dz % NZ])

    partner = (g, z * 2 + o)

    local = []

    def load(src, dst):
        cp = pltpu.make_async_copy(src, dst, lsem.at[len(local)])
        cp.start()
        local.append(cp)
        return cp

    ld_w = [load(wg_hbm, wgv), load(wu_hbm, wuv), load(wd_hbm, wdv), load(bas_hbm, basv)]
    ld_t = [load(tok_hbm, toks.at[c]), load(cot_hbm, cots.at[c])]
    ld_m = [load(fm_hbm, fmv), load(sm_hbm, smv)]

    barrier = pltpu.get_barrier_semaphore()
    near = [partner, dev(dx=1), dev(dx=-1), dev(dx=2), dev(dy=1), dev(dy=-1), dev(dy=2)]
    near += [dev(dz=e * t) for t in PLAN[0] for e in (1, -1)]

    for d in near:
        pl.semaphore_signal(barrier, inc=1, device_id=d, device_id_type=MESH)

    lead = Pool(lead_sem, NLEAD, partner)
    both = Pool(both_sem, NBOTH, partner)
    helper = Pool(help_sem, NHELP, partner)
    gather = Pool(gather_sem, NGATHER, partner)

    def chunk():
        return wbuf.at[0, pl.ds(0, 16)]

    def part():
        return lsend.at[:, pl.ds(0, NZ)]


    def arrived(dst, recv):
        pltpu.make_async_remote_copy(
            src_ref=dst, dst_ref=dst, send_sem=both_sem.at[0], recv_sem=recv,
            device_id=partner, device_id_type=MESH,
        ).wait_recv()

    def al(v, n):
        return pl.multiple_of(v, n)

    def roff(h, e=0):
        return al(xrows[e % NX] if h == 0 else yrows[e % NY], 16)

    pr = lax.broadcasted_iota(jnp.int32, (RANK, RANK), 0)
    pc = lax.broadcasted_iota(jnp.int32, (RANK, RANK), 1)
    perm = (pr == (pc & (NZ - 1)) * NP + (pc >> 4)).astype(F32).astype(BF)
    for cp in ld_w:
        cp.wait()
    bas = basv[...]
    bh = bas.astype(BF)
    bl = (bas - bh.astype(F32)).astype(BF)
    bp[c, 0] = jnp.dot(bh, perm, preferred_element_type=F32).astype(BF)
    bp[c, 1] = jnp.dot(bl, perm, preferred_element_type=F32).astype(BF)
    own_rows = pl.ds(al(c * ROWS, ROWS), ROWS)
    for half, put in ((o, "partner"), (c, "own")):
        fs = pl.ds(al(half * HF, HF), HF)
        rs = pl.ds(al(half * HR, HR), HR)
        for col, width, val in (
            (G0, HF, wgv[:, fs]), (U0, HF, wuv[:, fs]), (B0, HR, bp[c, 0, :, rs]), (D0, HF, wdv[:, fs]),
        ):
            if put == "partner":
                pk[:, col : col + width] = val
            else:
                wbuf[z, own_rows, col : col + width] = val

    pl.semaphore_wait(barrier, len(near))

    both.start(pk, wbuf.at[z, own_rows], psem.at[0], partner)

    def held(zo, row):
        return wbuf.at[zo, pl.ds(row, 16)]

    def zsend(zo, h, row, dz, rel):
        gather.start(held(zo, row), held(zo, row), zsem.at[h, rel], dev(dz=dz), chunk)

    own_off = al((1 - c) * xrows[0] + c * yrows[0], 16)
    oth_off = al(c * xrows[0] + (1 - c) * yrows[0], 16)
    for h, off in ((c, own_off), (o, oth_off)):
        if h is o:
            arrived(wbuf.at[z, pl.ds(al(o * ROWS, ROWS), ROWS)], psem.at[0])
        for t in PLAN[0]:
            zsend(z, h, off, t, t)
            zsend(z, h, off, -t, NZ - t)

    for cp in ld_t:
        cp.wait()
    both.start(toks.at[c], toks.at[c], psem.at[1], partner)
    both.start(cots.at[c], cots.at[c], psem.at[2], partner)

    for cp in ld_m:
        cp.wait()
    prow = lax.rem(p, 8)
    pcore = lax.div(p, 8)
    msend[6:8, :] = jnp.zeros((2, FF), F32)
    for i, mv in enumerate((fmv, smv)):
        for k in range(3):
            msend[3 * i + k : 3 * i + k + 1, :] = mv[k, pl.ds(prow, 1), :]

    @pl.when(helps)
    def _():
        helper.start(bp.at[0], bp.at[0], psem.at[3], partner, lambda: bp.at[0])
        helper.start(msend, mrecv, psem.at[4], partner)

    def origin(rel):
        return zs[-rel % NZ]

    def aside(h, e):
        return dev(dx=e) if h == 0 else dev(dy=e)

    def z_arrive(s):
        later = PLAN.get(s, ())
        for h in (0, 1):
            for d in (0, 1) if s < 8 else (h,):
                rel = s if d == 0 else NZ - s
                sgn = 1 if d == 0 else -1
                arrived(held(origin(rel), roff(h)), zsem.at[h, rel])
                for t in later[:1]:
                    if t < 8 or h == d:
                        zsend(origin(rel), h, roff(h), sgn * (t - s), (rel + sgn * (t - s)) % NZ)
        for h in (0, 1):
            for d in (0, 1):
                rel = s if d == 0 else NZ - s
                sgn = 1 if d == 0 else -1
                for t in later[1:]:
                    zsend(origin(rel), h, roff(h), sgn * (t - s), (rel + sgn * (t - s)) % NZ)

    def xy_send(s):
        for d in (0, 1):
            rel = s if d == 0 else NZ - s
            for h in (0, 1) if s < 8 else (d,):
                there = held(origin(rel), roff(h))
                for e in (2, 1, -1) if s in DIRECT else (1, -1):
                    way = {1: 0, -1: 1, 2: 2}[e]
                    gather.start(there, there, xysem.at[h, way, rel], aside(h, e), chunk)

    def pieces(s):
        if s == 8:
            return [(8, (0, 1))]
        return [(s, (0, 0)), (NZ - s, (1, 1))]

    def xy_direct(s):
        for rel, ways in pieces(s):
            for h in (0, 1):
                e = -1 if ways[h] == 0 else 1
                ch = held(origin(rel), roff(h, e))
                arrived(ch, xysem.at[h, ways[h], rel])
                if s not in DIRECT:
                    gather.start(ch, ch, xysem.at[h, 2, rel], aside(h, -e), chunk)

    def xy_rest(s):
        for rel, ways in pieces(s):
            for h in (0, 1):
                way = 1 - ways[h]
                e = -1 if way == 0 else 1
                arrived(held(origin(rel), roff(h, e)), xysem.at[h, way, rel])
                arrived(held(origin(rel), roff(h, 2)), xysem.at[h, 2, rel])

    def multiply(rel, first=False):
        zo = origin(rel)
        cols = pl.ds(al(zo * 128, 128), 128)
        tk = toks[:, :, cols].reshape(2 * TOK, 128)
        ck = cots[:, :, cols].reshape(2 * TOK, 128)
        ax = jnp.dot(tk, wbuf[zo, :, 0:D0], preferred_element_type=F32)
        ay = jnp.dot(ck, wbuf[zo, :, B0:PW], preferred_element_type=F32)
        if first:
            accx[...] = ax
            accy[...] = ay
        else:
            accx[...] += ax
            accy[...] += ay

    def finish(s):
        xy_rest(s)
        for rel, _ in pieces(s):
            multiply(rel)

    order = (2, 1, 4, 3, 6, 5, 8, 7)
    for i in range(0, 8, 2):
        for s in order[i : i + 2]:
            z_arrive(s)
            xy_send(s)
        if i == 0:
            arrived(toks.at[o], psem.at[1])
            arrived(cots.at[o], psem.at[2])
            multiply(0, first=True)
        else:
            for s in order[i - 2 : i]:
                xy_direct(s)
        if i > 2:
            for s in order[i - 4 : i - 2]:
                finish(s)

    @pl.when(leads)
    def _():
        arrived(mrecv, psem.at[4])
        mbuf[z] = jnp.where(pcore == 1, msend[...], mrecv[...])
        for dz in range(1, NZ):
            lead.start(mbuf.at[z], mbuf.at[z], msem.at[dz], dev(dz=dz, lead=True), lambda: mbuf.at[0])

    for s in order[6:8]:
        xy_direct(s)
    for s in order[4:8]:
        finish(s)

    hc = pl.ds(al(c * HR, HR), HR)
    ho = pl.ds(al(o * HR, HR), HR)
    xpb[0, :, hc] = accx[:, B0 : B0 + HR].astype(BF)
    xpb[1, :, hc] = accy[:, 0:HR].astype(BF)
    both.start(xpb.at[:, :, hc], xpb.at[:, :, hc], psem.at[5], partner)
    gate = accx[:, G0 : G0 + HF]
    up = accx[:, U0 : U0 + HF]
    dhid = accy[:, HR : HR + HF]
    sig = jax.nn.sigmoid(gate)
    silu = gate * sig
    hid[...] = (silu * up).astype(BF)
    dgu[:, 0:HF] = (dhid * up * sig * (1.0 + gate * (1.0 - sig))).astype(BF)
    dgu[:, HF : 2 * HF] = (dhid * silu).astype(BF)
    plane = [(dx, dy) for dy in range(NY) for dx in range(NX) if (dx, dy) != (0, 0)]
    far_first = sorted(plane, key=lambda t: -(min(t[0], NX - t[0]) + min(t[1], NY - t[1])))

    def back(dx, dy):
        return ((-dy) % NY) * NX + (-dx) % NX

    def part_of(dx, dy):
        return groups[dx, dy]

    def rows_of(q):
        return pl.ds(al(q * NZ, NZ), NZ)

    over_rows = (((0,), (0,)), ((), ()))
    parted = []
    for turn, hh in enumerate((c, o)):
        ranks = hc if turn == 0 else ho
        if turn == 1:
            arrived(xpb.at[:, :, ho], psem.at[5])
        l01 = lax.dot_general(xpb[0, :, ranks], dgu[...], over_rows, preferred_element_type=F32)
        lsend[0, ranks, :] = l01[:, 0:HF].astype(BF)
        lsend[1, ranks, :] = l01[:, HF : 2 * HF].astype(BF)
        lsend[2, ranks, :] = lax.dot_general(
            xpb[1, :, ranks], hid[...], over_rows, preferred_element_type=F32
        ).astype(BF)
        for i in range(8):
            q = hh * 8 + lax.rem(p + i, 8)
            away = jnp.logical_or(helps, q != p)
            parted.append(away)

            @pl.when(away)
            def _():
                pltpu.make_async_remote_copy(
                    src_ref=lsend.at[:, rows_of(q)], dst_ref=lrecv.at[p, c],
                    send_sem=part_sem.at[8 * turn + i], recv_sem=rsem.at[c, p],
                    device_id=(q, leaders[0]), device_id_type=MESH,
                ).start()

    @pl.when(leads)
    def _():
        lrecv[p, 1] = lsend[:, rows_of(p)]

    def dx_part(core, put):
        lhs = dgu[pl.ds(al(core * TOK, TOK), TOK), :]

        @pl.loop(0, NZ)
        def _(i):
            put(pl.ds(al(i * 128, 128), 128), lax.dot_general(
                lhs, wbuf[i, :, 0 : 2 * HF], (((1,), (1,)), ((), ())), preferred_element_type=F32
            ))

    def put_partner(cols, val):
        dxp[:, cols] = val

    def put_own(cols, val):
        dxo[:, cols] = (val + dxr[:, cols]).astype(BF)

    dx_part(o, put_partner)
    both.start(dxp, dxr, psem.at[6], partner)

    @pl.when(leads)
    def _():
        for half in (0, 1):
            for dx, dy in plane:
                arrived(lrecv.at[part_of(dx, dy), half], rsem.at[half, part_of(dx, dy)])
        arrived(lrecv.at[p, 0], rsem.at[0, p])
        total = lrecv[0].astype(F32)
        for q in range(1, NP):
            total = total + lrecv[q].astype(F32)
        t0b[...] = total.astype(BF)
        for i, dz in enumerate((1, -1, -2)):
            lead.start(t0b, nearb.at[i], nsem.at[i], dev(dz=dz, lead=True))
        for i in range(3):
            arrived(nearb.at[i], nsem.at[i])
        for i in range(3):
            total = total + nearb[i].astype(F32)
        t1b[...] = total.astype(BF)
        for i, dz in ((2, 8), (0, 4), (1, -4)):
            lead.start(t1b, farb.at[i], fsem.at[i], dev(dz=dz, lead=True))
        tv[...] = total

    arrived(dxr, psem.at[6])
    dx_part(c, put_own)
    def adam(low, first, second, factor):
        grad = factor * low
        nf = 0.5 * first + 0.5 * grad
        ns = 0.9 * second + 0.1 * grad * grad
        return nf, ns

    def factor_of(ssum):
        return jnp.minimum(1.0, EPS_LIMIT / jnp.sqrt(ssum + 1e-06))

    halves = (slice(0, HF), slice(HF, FF))

    def moments(low):
        factor = factor_of(sfac[0:1, :])
        for k in range(3):
            nf, ns = adam(low(k), fmv[k], smv[k], jnp.concatenate([factor, factor], axis=1))
            nfv[k] = nf
            nsv[k] = ns

    @pl.when(leads)
    def _():
        for i in range(3):
            arrived(farb.at[i], fsem.at[i])
        total = tv[...]
        for i in range(3):
            total = total + farb[i].astype(F32)
        flat = total.reshape(6 * NZ, HF)
        sq = jnp.sum(jnp.sum(flat * flat, axis=0, keepdims=True), axis=1, keepdims=True)
        sqb[p] = jnp.broadcast_to(sq, (1, HF))
        for dx, dy in far_first:
            lead.start(sqb.at[p], sqb.at[p], qsem.at[back(dx, dy)], dev(dx=dx, dy=dy, lead=True), lambda: sqb.at[0])
        zrow = lax.broadcasted_iota(jnp.int32, (3, NZ, HF), 1) == z
        lrow[3:8, :] = jnp.zeros((5, FF), F32)
        for half in (0, 1):
            lrow[0:3, halves[half]] = jnp.sum(jnp.where(zrow, total[half], 0.0), axis=1)
        lall[p] = lrow[...]
        for dx, dy in far_first:
            lead.start(lrow, lall.at[p], rowsem.at[back(dx, dy)], dev(dx=dx, dy=dy, lead=True))
        for dz in range(1, NZ):
            arrived(mbuf.at[origin(dz)], msem.at[dz])
        for dx, dy in plane:
            arrived(sqb.at[part_of(dx, dy)], qsem.at[dy * NX + dx])
        ssum = sqb[0]
        for q in range(1, NP):
            ssum = ssum + sqb[q]
        sfac[0:1, :] = ssum
        factor = factor_of(ssum)
        for k in range(3):
            for half in (0, 1):
                nf, ns = adam(total[half, k], mbuf[:, k, halves[half]], mbuf[:, 3 + k, halves[half]], factor)
                sbuf[k, rows_of(p), halves[half]] = (nf / (jnp.sqrt(ns) + 1e-08)).astype(BF)
        mine = sbuf.at[:, rows_of(p)]
        for dx, dy in far_first:
            lead.start(mine, mine, stsem.at[back(dx, dy)], dev(dx=dx, dy=dy, lead=True), lambda: sbuf.at[:, pl.ds(0, NZ)])
        for dx, dy in plane:
            arrived(lall.at[part_of(dx, dy)], rowsem.at[dy * NX + dx])
        lead.start(sfac, sfac, psem.at[8], partner)
        lead.start(lall.at[0:8], loth, psem.at[10], partner, lambda: lall.at[0:8])
        moments(lambda k: lall[8:16, k, :])

    @pl.when(helps)
    def _():
        arrived(sfac, psem.at[8])
        arrived(loth, psem.at[10])
        moments(lambda k: loth[:, k, :])

    def update(core, k):
        st = sbuf[k]
        return jnp.dot(bp[core, 0], st, preferred_element_type=F32) + jnp.dot(
            bp[core, 1], st, preferred_element_type=F32
        )

    @pl.when(leads)
    def _():
        arrived(bp.at[0], psem.at[3])
        for dx, dy in plane:
            arrived(sbuf.at[:, rows_of(part_of(dx, dy))], stsem.at[dy * NX + dx])
        for k in range(3):
            uov[k] = update(0, k)
        lead.start(uov, upv, psem.at[9], partner)
        for k in range(3):
            upv[k] = update(1, k)
        lead.drain()

    @pl.when(helps)
    def _():
        arrived(upv, psem.at[9])
        helper.drain()

    both.drain()
    gather.drain()
    for i, away in enumerate(parted):

        @pl.when(away)
        def _():
            pltpu.make_async_remote_copy(
                src_ref=part(), dst_ref=part(), send_sem=part_sem.at[i], recv_sem=rsem.at[0, 0],
                device_id=partner, device_id_type=MESH,
            ).wait_send()


def local(tokens, cotangent, w_gate, w_up, w_down, basis, first_moment, second_moment):
    anywhere = pl.BlockSpec(memory_space=pl.ANY)
    dma = pltpu.SemaphoreType.DMA
    v = pltpu.VMEM
    part = (2, 3, NZ, HF)
    scratch = [
        v((2, TOK, D), BF), v((2, TOK, D), BF), v((NZ, 128, PW), BF),
        v((ROWS, FF), BF), v((ROWS, FF), BF), v((ROWS, FF), BF), v((ROWS, RANK), F32),
        v((3, 8, FF), F32), v((3, 8, FF), F32),
        v((ROWS, PW), BF), v((2, 2, ROWS, RANK), BF),
        v((8, FF), F32), v((8, FF), F32), v((NZ, 8, FF), F32),
        v((2 * TOK, D0), F32), v((2 * TOK, HR + HF), F32),
        v((2, 2 * TOK, RANK), BF), v((2 * TOK, 2 * HF), BF), v((2 * TOK, HF), BF),
        v((3, RANK, HF), BF), v((NP, *part), BF),
        v((TOK, D), F32), v((TOK, D), F32),
        v(part, F32), v(part, BF), v((3, *part), BF), v(part, BF), v((3, *part), BF),
        v((NP, 1, HF), F32), v((8, HF), F32),
        v((8, FF), F32), v((NP, 8, FF), F32), v((8, 8, FF), F32),
        v((3, RANK, FF), BF), v((3, ROWS, FF), F32),
        dma((8,)), dma((NLEAD,)), dma((NBOTH,)), dma((NHELP,)), dma((NGATHER,)), dma((NP,)), dma((2, NZ)), dma((2, 3, NZ)), dma((11,)),
        dma((NZ,)), dma((2, NP)), dma((3,)), dma((3,)), dma((NP,)), dma((NP,)), dma((NP,)),
    ]
    kept = [((TOK, D), BF), ((3, 8, FF), F32), ((3, 8, FF), F32), ((3, ROWS, FF), F32)]
    inside = pl.BlockSpec(memory_space=pltpu.VMEM)
    results = pl.pallas_call(
        kernel,
        out_shape=tuple(pltpu.VMEM(*k) for k in kept),
        in_specs=[anywhere] * 8,
        out_specs=(inside,) * 4,
        scratch_shapes=scratch,
        compiler_params=pltpu.CompilerParams(
            collective_id=0, has_side_effects=True, vmem_limit_bytes=58 * 1024 * 1024
        ),
    )(tokens, cotangent, w_gate, w_up, w_down, basis, first_moment, second_moment)
    return pl.pallas_call(
        put_out,
        out_shape=tuple(jax.ShapeDtypeStruct(*k) for k in kept),
        in_specs=[inside] * 4,
        out_specs=(anywhere,) * 4,
        scratch_shapes=[dma((4,))],
        compiler_params=pltpu.CompilerParams(vmem_limit_bytes=4 * 1024 * 1024),
    )(*results)


def put_out(a, b, c, d, a_hbm, b_hbm, c_hbm, d_hbm, sem):
    pairs = ((a, a_hbm), (b, b_hbm), (c, c_hbm), (d, d_hbm))
    copies = [pltpu.make_async_copy(src, dst, sem.at[i]) for i, (src, dst) in enumerate(pairs)]
    for cp in copies:
        cp.start()
    for cp in copies:
        cp.wait()


def solution(mesh):
    both = ("group", "member")
    placed = (
        P(both, None), P(both, None), P("member", None), P("member", None), P("member", None),
        P("member", None), P(None, "member", None), P(None, "member", None),
    )
    return jax.shard_map(
        local,
        mesh=mesh,
        in_specs=placed,
        out_specs=(P(both, None), P(None, "member", None), P(None, "member", None), P(None, "member", None)),
        check_vma=False,
    )
```

```python
import functools
import math

import jax
import jax.numpy as jnp
from jax import lax
from jax.experimental import pallas as pl
from jax.experimental.pallas import tpu as pltpu
from jax.sharding import PartitionSpec as P

BF = jnp.bfloat16
F32 = jnp.float32
MESH = pl.DeviceIdType.MESH

D = 2048
FF = 512
RANK = 256
TOK = 128
NX, NY, NZ = 4, 4, 16
NP = NX * NY
HF = FF // 2
HR = RANK // 2
ROWS = 64
PW = 3 * HF + HR
EPS_LIMIT = math.sqrt(3.0 * RANK * FF)

G0, U0, B0, D0 = 0, HF, 2 * HF, 2 * HF + HR


class Pool:
    def __init__(self, ref, count, near):
        self.ref, self.count, self.near, self.started, self.done = ref, count, near, [], 0

    def start(self, src, dst, recv, device, like=None):
        if len(self.started) - self.done == self.count:
            self.wait_oldest(recv)
        pltpu.make_async_remote_copy(
            src_ref=src, dst_ref=dst, send_sem=self.ref.at[len(self.started) % self.count],
            recv_sem=recv, device_id=device, device_id_type=MESH,
        ).start()
        self.started.append(src if like is None else like)

    def wait_oldest(self, recv):
        like = self.started[self.done]
        like = like() if callable(like) else like
        pltpu.make_async_remote_copy(
            src_ref=like, dst_ref=like, send_sem=self.ref.at[self.done % self.count],
            recv_sem=recv, device_id=self.near, device_id_type=MESH,
        ).wait_send()
        self.done += 1

    def drain(self):
        while self.done < len(self.started):
            self.wait_oldest(self.ref.at[0])


NLEAD, NBOTH, NHELP, NGATHER = 72, 24, 8, 160

PLAN = {0: (2, 1), 2: (4, 3), 4: (6, 5), 6: (8, 7)}
DIRECT = (7, 8)


def kernel(
    tok_hbm, cot_hbm, wg_hbm, wu_hbm, wd_hbm, bas_hbm, fm_hbm, sm_hbm,
    dxo, nfv, nsv, upv,
    toks, cots, wbuf, wgv, wuv, wdv, basv, fmv, smv,
    pk, bp, msend, mrecv, mbuf,
    accx, accy, xpb, dgu, hid, lsend, lrecv,
    dxp, dxr, tv, t0b, nearb, t1b, farb,
    sqb, sfac, lrow, lall, loth, sbuf, uov,
    lsem, lead_sem, both_sem, help_sem, gather_sem, part_sem, zsem, xysem, psem, msem, rsem, nsem, fsem, qsem, rowsem, stsem,
):
    g = lax.axis_index("group")
    m = lax.axis_index("member")
    y, x = lax.div(g, NX), lax.rem(g, NX)
    z, c = lax.div(m, 2), lax.rem(m, 2)
    o = 1 - c
    p = g
    leads, helps = c == 1, c == 0

    xs = [x] + [lax.rem(x + d, NX) for d in range(1, NX)]
    ys = [y] + [lax.rem(y + d, NY) for d in range(1, NY)]
    zs = [z] + [lax.rem(z + d, NZ) for d in range(1, NZ)]
    groups = {(i, j): ys[j] * NX + xs[i] for i in range(NX) for j in range(NY)}
    groups[0, 0] = g
    members = [zs[i] * 2 + c for i in range(NZ)]
    leaders = [zs[i] * 2 + 1 for i in range(NZ)]
    xrows = [16 * xs[i] for i in range(NX)]
    yrows = [64 + 16 * ys[i] for i in range(NY)]

    def dev(dx=0, dy=0, dz=0, lead=False):
        return (groups[dx % NX, dy % NY], (leaders if lead else members)[dz % NZ])

    partner = (g, z * 2 + o)

    local = []

    def load(src, dst):
        cp = pltpu.make_async_copy(src, dst, lsem.at[len(local)])
        cp.start()
        local.append(cp)
        return cp

    ld_w = [load(wg_hbm, wgv), load(wu_hbm, wuv), load(wd_hbm, wdv), load(bas_hbm, basv)]
    ld_t = [load(tok_hbm, toks.at[c]), load(cot_hbm, cots.at[c])]
    ld_m = [load(fm_hbm, fmv), load(sm_hbm, smv)]

    barrier = pltpu.get_barrier_semaphore()
    near = [partner, dev(dx=1), dev(dx=-1), dev(dx=2), dev(dy=1), dev(dy=-1), dev(dy=2)]
    near += [dev(dz=e * t) for t in PLAN[0] for e in (1, -1)]

    for d in near:
        pl.semaphore_signal(barrier, inc=1, device_id=d, device_id_type=MESH)

    lead = Pool(lead_sem, NLEAD, partner)
    both = Pool(both_sem, NBOTH, partner)
    helper = Pool(help_sem, NHELP, partner)
    gather = Pool(gather_sem, NGATHER, partner)

    def chunk():
        return wbuf.at[0, pl.ds(0, 16)]

    def part():
        return lsend.at[:, pl.ds(0, NZ)]


    def arrived(dst, recv):
        pltpu.make_async_remote_copy(
            src_ref=dst, dst_ref=dst, send_sem=both_sem.at[0], recv_sem=recv,
            device_id=partner, device_id_type=MESH,
        ).wait_recv()

    def al(v, n):
        return pl.multiple_of(v, n)

    def roff(h, e=0):
        return al(xrows[e % NX] if h == 0 else yrows[e % NY], 16)

    pr = lax.broadcasted_iota(jnp.int32, (RANK, RANK), 0)
    pc = lax.broadcasted_iota(jnp.int32, (RANK, RANK), 1)
    perm = (pr == (pc & (NZ - 1)) * NP + (pc >> 4)).astype(F32).astype(BF)
    for cp in ld_w:
        cp.wait()
    bas = basv[...]
    bh = bas.astype(BF)
    bl = (bas - bh.astype(F32)).astype(BF)
    bp[c, 0] = jnp.dot(bh, perm, preferred_element_type=F32).astype(BF)
    bp[c, 1] = jnp.dot(bl, perm, preferred_element_type=F32).astype(BF)
    own_rows = pl.ds(al(c * ROWS, ROWS), ROWS)
    for half, put in ((o, "partner"), (c, "own")):
        fs = pl.ds(al(half * HF, HF), HF)
        rs = pl.ds(al(half * HR, HR), HR)
        for col, width, val in (
            (G0, HF, wgv[:, fs]), (U0, HF, wuv[:, fs]), (B0, HR, bp[c, 0, :, rs]), (D0, HF, wdv[:, fs]),
        ):
            if put == "partner":
                pk[:, col : col + width] = val
            else:
                wbuf[z, own_rows, col : col + width] = val

    pl.semaphore_wait(barrier, len(near))

    both.start(pk, wbuf.at[z, own_rows], psem.at[0], partner)

    def held(zo, row):
        return wbuf.at[zo, pl.ds(row, 16)]

    def zsend(zo, h, row, dz, rel):
        gather.start(held(zo, row), held(zo, row), zsem.at[h, rel], dev(dz=dz), chunk)

    own_off = al((1 - c) * xrows[0] + c * yrows[0], 16)
    oth_off = al(c * xrows[0] + (1 - c) * yrows[0], 16)
    for h, off in ((c, own_off), (o, oth_off)):
        if h is o:
            arrived(wbuf.at[z, pl.ds(al(o * ROWS, ROWS), ROWS)], psem.at[0])
        for t in PLAN[0]:
            zsend(z, h, off, t, t)
            zsend(z, h, off, -t, NZ - t)

    for cp in ld_t:
        cp.wait()
    both.start(toks.at[c], toks.at[c], psem.at[1], partner)
    both.start(cots.at[c], cots.at[c], psem.at[2], partner)

    for cp in ld_m:
        cp.wait()
    prow = lax.rem(p, 8)
    pcore = lax.div(p, 8)
    msend[6:8, :] = jnp.zeros((2, FF), F32)
    for i, mv in enumerate((fmv, smv)):
        for k in range(3):
            msend[3 * i + k : 3 * i + k + 1, :] = mv[k, pl.ds(prow, 1), :]

    @pl.when(helps)
    def _():
        helper.start(bp.at[0], bp.at[0], psem.at[3], partner, lambda: bp.at[0])
        helper.start(msend, mrecv, psem.at[4], partner)

    def origin(rel):
        return zs[-rel % NZ]

    def aside(h, e):
        return dev(dx=e) if h == 0 else dev(dy=e)

    def z_arrive(s):
        later = PLAN.get(s, ())
        for h, row in ((c, own_off), (o, oth_off)) if s < 6 else ((0, roff(0)), (1, roff(1))):
            for d in (0, 1) if s < 8 else (h,):
                rel = s if d == 0 else NZ - s
                sgn = 1 if d == 0 else -1
                arrived(held(origin(rel), row), zsem.at[h, rel])
                for t in later[:1]:
                    if s < 6 or t < 8 or h == d:
                        zsend(origin(rel), h, row, sgn * (t - s), (rel + sgn * (t - s)) % NZ)
        for h in (0, 1):
            for d in (0, 1):
                rel = s if d == 0 else NZ - s
                sgn = 1 if d == 0 else -1
                for t in later[1:]:
                    zsend(origin(rel), h, roff(h), sgn * (t - s), (rel + sgn * (t - s)) % NZ)

    def xy_send(s):
        for d in (0, 1):
            rel = s if d == 0 else NZ - s
            for h in (0, 1) if s < 8 else (d,):
                there = held(origin(rel), roff(h))
                for e in (2, 1, -1) if s in DIRECT else (1, -1):
                    way = {1: 0, -1: 1, 2: 2}[e]
                    gather.start(there, there, xysem.at[h, way, rel], aside(h, e), chunk)

    def pieces(s):
        if s == 8:
            return [(8, (0, 1))]
        return [(s, (0, 0)), (NZ - s, (1, 1))]

    def xy_direct(s):
        for rel, ways in pieces(s):
            for h in (0, 1):
                e = -1 if ways[h] == 0 else 1
                ch = held(origin(rel), roff(h, e))
                arrived(ch, xysem.at[h, ways[h], rel])
                if s not in DIRECT:
                    gather.start(ch, ch, xysem.at[h, 2, rel], aside(h, -e), chunk)

    def xy_rest(s):
        for rel, ways in pieces(s):
            for h in (0, 1):
                way = 1 - ways[h]
                e = -1 if way == 0 else 1
                arrived(held(origin(rel), roff(h, e)), xysem.at[h, way, rel])
                arrived(held(origin(rel), roff(h, 2)), xysem.at[h, 2, rel])

    def multiply(rel, first=False):
        zo = origin(rel)
        cols = pl.ds(al(zo * 128, 128), 128)
        tk = toks[:, :, cols].reshape(2 * TOK, 128)
        ck = cots[:, :, cols].reshape(2 * TOK, 128)
        ax = jnp.dot(tk, wbuf[zo, :, 0:D0], preferred_element_type=F32)
        ay = jnp.dot(ck, wbuf[zo, :, B0:PW], preferred_element_type=F32)
        if first:
            accx[...] = ax
            accy[...] = ay
        else:
            accx[...] += ax
            accy[...] += ay

    def finish(s):
        xy_rest(s)
        for rel, _ in pieces(s):
            multiply(rel)

    order = (2, 1, 4, 3, 6, 5, 8, 7)
    for i in range(0, 8, 2):
        for s in order[i : i + 2]:
            z_arrive(s)
            xy_send(s)
        if i == 0:
            arrived(toks.at[o], psem.at[1])
            arrived(cots.at[o], psem.at[2])
            multiply(0, first=True)
        else:
            for s in order[i - 2 : i]:
                xy_direct(s)
        if i > 2:
            for s in order[i - 4 : i - 2]:
                finish(s)

    @pl.when(leads)
    def _():
        arrived(mrecv, psem.at[4])
        mbuf[z] = jnp.where(pcore == 1, msend[...], mrecv[...])
        for dz in range(1, NZ):
            lead.start(mbuf.at[z], mbuf.at[z], msem.at[dz], dev(dz=dz, lead=True), lambda: mbuf.at[0])

    for s in order[6:8]:
        xy_direct(s)
    for s in order[4:8]:
        finish(s)

    hc = pl.ds(al(c * HR, HR), HR)
    ho = pl.ds(al(o * HR, HR), HR)
    xpb[0, :, hc] = accx[:, B0 : B0 + HR].astype(BF)
    xpb[1, :, hc] = accy[:, 0:HR].astype(BF)
    both.start(xpb.at[:, :, hc], xpb.at[:, :, hc], psem.at[5], partner)
    gate = accx[:, G0 : G0 + HF]
    up = accx[:, U0 : U0 + HF]
    dhid = accy[:, HR : HR + HF]
    sig = jax.nn.sigmoid(gate)
    silu = gate * sig
    hid[...] = (silu * up).astype(BF)
    dgu[:, 0:HF] = (dhid * up * sig * (1.0 + gate * (1.0 - sig))).astype(BF)
    dgu[:, HF : 2 * HF] = (dhid * silu).astype(BF)
    plane = [(dx, dy) for dy in range(NY) for dx in range(NX) if (dx, dy) != (0, 0)]
    far_first = sorted(plane, key=lambda t: -(min(t[0], NX - t[0]) + min(t[1], NY - t[1])))

    def back(dx, dy):
        return ((-dy) % NY) * NX + (-dx) % NX

    def part_of(dx, dy):
        return groups[dx, dy]

    def rows_of(q):
        return pl.ds(al(q * NZ, NZ), NZ)

    over_rows = (((0,), (0,)), ((), ()))
    parted = []
    for turn, hh in enumerate((c, o)):
        ranks = hc if turn == 0 else ho
        if turn == 1:
            arrived(xpb.at[:, :, ho], psem.at[5])
        l01 = lax.dot_general(xpb[0, :, ranks], dgu[...], over_rows, preferred_element_type=F32)
        lsend[0, ranks, :] = l01[:, 0:HF].astype(BF)
        lsend[1, ranks, :] = l01[:, HF : 2 * HF].astype(BF)
        lsend[2, ranks, :] = lax.dot_general(
            xpb[1, :, ranks], hid[...], over_rows, preferred_element_type=F32
        ).astype(BF)
        for i in range(8):
            q = hh * 8 + lax.rem(p + i, 8)
            away = jnp.logical_or(helps, q != p)
            parted.append(away)

            @pl.when(away)
            def _():
                pltpu.make_async_remote_copy(
                    src_ref=lsend.at[:, rows_of(q)], dst_ref=lrecv.at[p, c],
                    send_sem=part_sem.at[8 * turn + i], recv_sem=rsem.at[c, p],
                    device_id=(q, leaders[0]), device_id_type=MESH,
                ).start()

    @pl.when(leads)
    def _():
        lrecv[p, 1] = lsend[:, rows_of(p)]

    def dx_part(core, put):
        lhs = dgu[pl.ds(al(core * TOK, TOK), TOK), :]

        @pl.loop(0, NZ)
        def _(i):
            put(pl.ds(al(i * 128, 128), 128), lax.dot_general(
                lhs, wbuf[i, :, 0 : 2 * HF], (((1,), (1,)), ((), ())), preferred_element_type=F32
            ))

    def put_partner(cols, val):
        dxp[:, cols] = val

    def put_own(cols, val):
        dxo[:, cols] = (val + dxr[:, cols]).astype(BF)

    dx_part(o, put_partner)
    both.start(dxp, dxr, psem.at[6], partner)

    @pl.when(leads)
    def _():
        for half in (0, 1):
            for dx, dy in plane:
                arrived(lrecv.at[part_of(dx, dy), half], rsem.at[half, part_of(dx, dy)])
        arrived(lrecv.at[p, 0], rsem.at[0, p])
        total = lrecv[0].astype(F32)
        for q in range(1, NP):
            total = total + lrecv[q].astype(F32)
        t0b[...] = total.astype(BF)
        for i, dz in enumerate((1, -1, -2)):
            lead.start(t0b, nearb.at[i], nsem.at[i], dev(dz=dz, lead=True))
        for i in range(3):
            arrived(nearb.at[i], nsem.at[i])
        for i in range(3):
            total = total + nearb[i].astype(F32)
        t1b[...] = total.astype(BF)
        for i, dz in ((2, 8), (0, 4), (1, -4)):
            lead.start(t1b, farb.at[i], fsem.at[i], dev(dz=dz, lead=True))
        tv[...] = total

    arrived(dxr, psem.at[6])
    dx_part(c, put_own)
    def adam(low, first, second, factor):
        grad = factor * low
        nf = 0.5 * first + 0.5 * grad
        ns = 0.9 * second + 0.1 * grad * grad
        return nf, ns

    def factor_of(ssum):
        return jnp.minimum(1.0, EPS_LIMIT / jnp.sqrt(ssum + 1e-06))

    halves = (slice(0, HF), slice(HF, FF))

    def moments(low):
        factor = factor_of(sfac[0:1, :])
        for k in range(3):
            nf, ns = adam(low(k), fmv[k], smv[k], jnp.concatenate([factor, factor], axis=1))
            nfv[k] = nf
            nsv[k] = ns

    @pl.when(leads)
    def _():
        for i in range(3):
            arrived(farb.at[i], fsem.at[i])
        total = tv[...]
        for i in range(3):
            total = total + farb[i].astype(F32)
        flat = total.reshape(6 * NZ, HF)
        sq = jnp.sum(jnp.sum(flat * flat, axis=0, keepdims=True), axis=1, keepdims=True)
        sqb[p] = jnp.broadcast_to(sq, (1, HF))
        for dx, dy in far_first:
            lead.start(sqb.at[p], sqb.at[p], qsem.at[back(dx, dy)], dev(dx=dx, dy=dy, lead=True), lambda: sqb.at[0])
        zrow = lax.broadcasted_iota(jnp.int32, (3, NZ, HF), 1) == z
        lrow[3:8, :] = jnp.zeros((5, FF), F32)
        for half in (0, 1):
            lrow[0:3, halves[half]] = jnp.sum(jnp.where(zrow, total[half], 0.0), axis=1)
        lall[p] = lrow[...]
        for dx, dy in far_first:
            lead.start(lrow, lall.at[p], rowsem.at[back(dx, dy)], dev(dx=dx, dy=dy, lead=True))
        for dz in range(1, NZ):
            arrived(mbuf.at[origin(dz)], msem.at[dz])
        for dx, dy in plane:
            arrived(sqb.at[part_of(dx, dy)], qsem.at[dy * NX + dx])
        ssum = sqb[0]
        for q in range(1, NP):
            ssum = ssum + sqb[q]
        sfac[0:1, :] = ssum
        factor = factor_of(ssum)
        for k in range(3):
            for half in (0, 1):
                nf, ns = adam(total[half, k], mbuf[:, k, halves[half]], mbuf[:, 3 + k, halves[half]], factor)
                sbuf[k, rows_of(p), halves[half]] = (nf / (jnp.sqrt(ns) + 1e-08)).astype(BF)
        mine = sbuf.at[:, rows_of(p)]
        for dx, dy in far_first:
            lead.start(mine, mine, stsem.at[back(dx, dy)], dev(dx=dx, dy=dy, lead=True), lambda: sbuf.at[:, pl.ds(0, NZ)])
        for dx, dy in plane:
            arrived(lall.at[part_of(dx, dy)], rowsem.at[dy * NX + dx])
        lead.start(sfac, sfac, psem.at[8], partner)
        lead.start(lall.at[0:8], loth, psem.at[10], partner, lambda: lall.at[0:8])
        moments(lambda k: lall[8:16, k, :])

    @pl.when(helps)
    def _():
        arrived(sfac, psem.at[8])
        arrived(loth, psem.at[10])
        moments(lambda k: loth[:, k, :])

    def update(core, k):
        st = sbuf[k]
        return jnp.dot(bp[core, 0], st, preferred_element_type=F32) + jnp.dot(
            bp[core, 1], st, preferred_element_type=F32
        )

    @pl.when(leads)
    def _():
        arrived(bp.at[0], psem.at[3])
        for dx, dy in plane:
            arrived(sbuf.at[:, rows_of(part_of(dx, dy))], stsem.at[dy * NX + dx])
        for k in range(3):
            uov[k] = update(0, k)
        lead.start(uov, upv, psem.at[9], partner)
        for k in range(3):
            upv[k] = update(1, k)
        lead.drain()

    @pl.when(helps)
    def _():
        arrived(upv, psem.at[9])
        helper.drain()

    both.drain()
    gather.drain()
    for i, away in enumerate(parted):

        @pl.when(away)
        def _():
            pltpu.make_async_remote_copy(
                src_ref=part(), dst_ref=part(), send_sem=part_sem.at[i], recv_sem=rsem.at[0, 0],
                device_id=partner, device_id_type=MESH,
            ).wait_send()


def local(tokens, cotangent, w_gate, w_up, w_down, basis, first_moment, second_moment):
    anywhere = pl.BlockSpec(memory_space=pl.ANY)
    dma = pltpu.SemaphoreType.DMA
    v = pltpu.VMEM
    part = (2, 3, NZ, HF)
    scratch = [
        v((2, TOK, D), BF), v((2, TOK, D), BF), v((NZ, 128, PW), BF),
        v((ROWS, FF), BF), v((ROWS, FF), BF), v((ROWS, FF), BF), v((ROWS, RANK), F32),
        v((3, 8, FF), F32), v((3, 8, FF), F32),
        v((ROWS, PW), BF), v((2, 2, ROWS, RANK), BF),
        v((8, FF), F32), v((8, FF), F32), v((NZ, 8, FF), F32),
        v((2 * TOK, D0), F32), v((2 * TOK, HR + HF), F32),
        v((2, 2 * TOK, RANK), BF), v((2 * TOK, 2 * HF), BF), v((2 * TOK, HF), BF),
        v((3, RANK, HF), BF), v((NP, *part), BF),
        v((TOK, D), F32), v((TOK, D), F32),
        v(part, F32), v(part, BF), v((3, *part), BF), v(part, BF), v((3, *part), BF),
        v((NP, 1, HF), F32), v((8, HF), F32),
        v((8, FF), F32), v((NP, 8, FF), F32), v((8, 8, FF), F32),
        v((3, RANK, FF), BF), v((3, ROWS, FF), F32),
        dma((8,)), dma((NLEAD,)), dma((NBOTH,)), dma((NHELP,)), dma((NGATHER,)), dma((NP,)), dma((2, NZ)), dma((2, 3, NZ)), dma((11,)),
        dma((NZ,)), dma((2, NP)), dma((3,)), dma((3,)), dma((NP,)), dma((NP,)), dma((NP,)),
    ]
    kept = [((TOK, D), BF), ((3, 8, FF), F32), ((3, 8, FF), F32), ((3, ROWS, FF), F32)]
    inside = pl.BlockSpec(memory_space=pltpu.VMEM)
    results = pl.pallas_call(
        kernel,
        out_shape=tuple(pltpu.VMEM(*k) for k in kept),
        in_specs=[anywhere] * 8,
        out_specs=(inside,) * 4,
        scratch_shapes=scratch,
        compiler_params=pltpu.CompilerParams(
            collective_id=0, has_side_effects=True, vmem_limit_bytes=58 * 1024 * 1024
        ),
    )(tokens, cotangent, w_gate, w_up, w_down, basis, first_moment, second_moment)
    return pl.pallas_call(
        put_out,
        out_shape=tuple(jax.ShapeDtypeStruct(*k) for k in kept),
        in_specs=[inside] * 4,
        out_specs=(anywhere,) * 4,
        scratch_shapes=[dma((4,))],
        compiler_params=pltpu.CompilerParams(vmem_limit_bytes=4 * 1024 * 1024),
    )(*results)


def put_out(a, b, c, d, a_hbm, b_hbm, c_hbm, d_hbm, sem):
    pairs = ((a, a_hbm), (b, b_hbm), (c, c_hbm), (d, d_hbm))
    copies = [pltpu.make_async_copy(src, dst, sem.at[i]) for i, (src, dst) in enumerate(pairs)]
    for cp in copies:
        cp.start()
    for cp in copies:
        cp.wait()


def solution(mesh):
    both = ("group", "member")
    placed = (
        P(both, None), P(both, None), P("member", None), P("member", None), P("member", None),
        P("member", None), P(None, "member", None), P(None, "member", None),
    )
    return jax.shard_map(
        local,
        mesh=mesh,
        in_specs=placed,
        out_specs=(P(both, None), P(None, "member", None), P(None, "member", None), P(None, "member", None)),
        check_vma=False,
    )
```
